32 devices in a mesh: shard: 8 (over y, x, core), tp: 4 (over z).
Axes of the slice: x: 2, y: 2, z: 4, core: 2. Of those that a mesh axis runs over, the one named last changes fastest.
Arguments:
- weight_gate: bfloat16 [2560, 9728], P('shard', 'tp'), may hold values from -0.15625 to 0.15625
- low_gate: bfloat16 [2560, 32], P('shard'), may hold values from -0.125 to 0.125
- high_gate: bfloat16 [32, 9728], P(None, 'tp'), may hold values from -1 to 1
- weight_up: bfloat16 [2560, 9728], P('shard', 'tp'), may hold values from -0.15625 to 0.15625
- low_up: bfloat16 [2560, 32], P('shard'), may hold values from -0.125 to 0.125
- high_up: bfloat16 [32, 9728], P(None, 'tp'), may hold values from -1 to 1
- norm_gain: float32 [2560], P('shard'), may hold values from 0.25 to 1.75
Outputs:
- ready_gate: bfloat16 [2560, 9728], P(None, 'tp')
- ready_up: bfloat16 [2560, 9728], P(None, 'tp')
- factor_gate: float32 [9728], P('tp')
- factor_up: float32 [9728], P('tp')
The draws below stay inside these ranges and needn't reach their ends.
All inputs are finite; a program needn't handle non-finite values.
Results may differ from the reference program's by a relative error of at most 0.001.
Values may be sent and summed in bfloat16 or wider, within the bound.
A program may use at most 128 MiB of HBM per device.

```python
import jax
import jax.numpy as jnp
from jax import lax

D_MODEL = 2560
D_INNER = 9728
RANK = 32


def spiked(result, rng, source, target, shards_of, factor):
    owner, partner = [(jnp.arange(result.shape[dim]) // (result.shape[dim] // shards_of)).reshape([-1 if axis == dim else 1 for axis in range(result.ndim)]) for dim in (source, target)]
    chosen = jax.random.permutation(rng, shards_of)[partner]
    strong = (owner == chosen) | (owner == (partner + shards_of // 2) % shards_of)
    return jnp.where(strong, factor * result, result)


def block_scale(stream_key, dims, split, low, largest):
    loudness, own = 1.0, jax.random.fold_in(stream_key, 6)
    for position, shards_of in split:
        draws = jnp.exp(jax.random.uniform(jax.random.fold_in(own, position), (shards_of,), jnp.float32, low / len(split), largest / len(split)))
        loudness = loudness * jnp.repeat(draws, dims[position] // shards_of).reshape([-1 if axis == position else 1 for axis in range(len(dims))])
    return loudness


def scatter_about(rng, shape, scale, most, shards=(), dtype=jnp.bfloat16):
    drawn = jax.random.normal(rng, shape, jnp.float32) * scale
    if len(shards) > 0:
        drawn = block_scale(rng, shape, shards, -0.22, 0.18) * drawn
    return jnp.clip(drawn, min=-most, max=most).astype(dtype)


def bell_draw_with(key, shape, scale, bound, shards, heavy, kind=jnp.bfloat16):
    array = scale * jax.random.normal(key, shape, jnp.float32)
    if shards:
        array = array * block_scale(key, shape, shards, -0.22, 0.18)
    return jnp.clip(spiked(array, jax.random.fold_in(key, 3), *heavy), -bound, bound).astype(kind)


def setup_inputs(seed: int = 0) -> dict:
    streams_of = jax.random.split(jax.random.key(seed), 8)
    return {
        "weight_gate": bell_draw_with(streams_of[0], (D_MODEL, D_INNER), D_MODEL ** -0.5, 0.15625, ((0, 8), (1, 4)), (0, 1, 8, 2.0)),
        "low_gate": scatter_about(streams_of[1], (D_MODEL, RANK), D_MODEL ** -0.5, 0.125, ((0, 8),)),
        "high_gate": scatter_about(streams_of[2], (RANK, D_INNER), RANK ** -0.5, 1.0, ((1, 4),)),
        "weight_up": bell_draw_with(streams_of[3], (D_MODEL, D_INNER), D_MODEL ** -0.5, 0.15625, ((0, 8), (1, 4)), (0, 1, 8, 2.0)),
        "low_up": scatter_about(streams_of[4], (D_MODEL, RANK), D_MODEL ** -0.5, 0.125, ((0, 8),)),
        "high_up": scatter_about(streams_of[5], (RANK, D_INNER), RANK ** -0.5, 1.0, ((1, 4),)),
        "norm_gain": jnp.clip(1.0 + 0.15 * jax.random.normal(streams_of[6], (D_MODEL,), jnp.float32), 0.25, 1.75),
    }


mix_rate = 2.0

def reference(weight_gate, low_gate, high_gate, weight_up, low_up, high_up, norm_gain):
    latest_gate = weight_gate.astype(jnp.float32) + mix_rate * jnp.dot(low_gate, high_gate, preferred_element_type=jnp.float32)
    latest_up = weight_up.astype(jnp.float32) + mix_rate * jnp.dot(low_up, high_up, preferred_element_type=jnp.float32)
    latest_gained_gate = latest_gate * norm_gain[:, None]
    latest_gained_up = latest_up * norm_gain[:, None]
    factor_gate = jnp.sqrt(lax.optimization_barrier(jnp.sum(latest_gained_gate * latest_gained_gate, axis=0)))
    ready_gate = (latest_gained_gate / factor_gate).astype(jnp.bfloat16)
    factor_up = jnp.sqrt(lax.optimization_barrier(jnp.sum(latest_gained_up * latest_gained_up, axis=0)))
    ready_up = (latest_gained_up / factor_up).astype(jnp.bfloat16)
    return (ready_gate, ready_up, factor_gate, factor_up)
```

```python
import functools
import math

import jax
import jax.numpy as jnp
from jax import lax
from jax.experimental import pallas as pl
from jax.experimental.pallas import tpu as pltpu
from jax.sharding import PartitionSpec as P

mix_rate = 2.0
AXIS = "shard"


def local(weight_gate, low_gate, high_gate, weight_up, low_up, high_up, norm_gain):
    latest_gate = weight_gate.astype(jnp.float32) + mix_rate * jnp.dot(
        low_gate, high_gate, preferred_element_type=jnp.float32
    )
    latest_up = weight_up.astype(jnp.float32) + mix_rate * jnp.dot(
        low_up, high_up, preferred_element_type=jnp.float32
    )
    latest_gained_gate = latest_gate * norm_gain[:, None]
    latest_gained_up = latest_up * norm_gain[:, None]
    total_gate, total_up = lax.psum(
        (
            jnp.sum(latest_gained_gate * latest_gained_gate, axis=0),
            jnp.sum(latest_gained_up * latest_gained_up, axis=0),
        ),
        AXIS,
    )
    factor_gate = jnp.sqrt(total_gate)
    factor_up = jnp.sqrt(total_up)
    narrow_gate = (latest_gained_gate / factor_gate).astype(jnp.bfloat16)
    narrow_up = (latest_gained_up / factor_up).astype(jnp.bfloat16)
    ready_gate = lax.all_gather(narrow_gate, AXIS, axis=0, tiled=True)
    ready_up = lax.all_gather(narrow_up, AXIS, axis=0, tiled=True)
    return (ready_gate, ready_up, factor_gate, factor_up)


def gather_kernel(
    n, chunks, raw, wg_hbm, wu_hbm, lg_hbm, lu_hbm, hg_hbm, hu_hbm, gain_hbm,
    out_g, out_u, fac,
    w_v, l_v, h_v, gain_v, low_v, g_v, col_v, sums, rf_v, far_low,
    in_sem, ssum, rsum, slow, rlow, send, recv,
):
    rows, cols = wg_hbm.shape
    step = rows // chunks
    me = lax.axis_index(AXIS)
    core = lax.rem(me, 2)
    x = lax.rem(me // 2, 2)
    y = me // 4
    sib = me + 1 - 2 * core
    to_x = me + 2 - 4 * x
    to_y = me + 4 - 8 * y
    diag = to_x + 4 - 8 * y

    barrier = pltpu.get_barrier_semaphore()
    for d in range(1, n):
        pl.semaphore_signal(barrier, inc=1, device_id={AXIS: lax.rem(me + d, n)})

    gain_load = pltpu.make_async_copy(gain_hbm, gain_v.at[0], in_sem.at[6])
    low_loads, high_loads, loads = (
        [
            pltpu.make_async_copy(src, dst.at[a], in_sem.at[3 * a + i])
            for a, src in enumerate(pair)
        ]
        for i, (pair, dst) in enumerate((
            ((lg_hbm, lu_hbm), l_v), ((hg_hbm, hu_hbm), h_v), ((wg_hbm, wu_hbm), w_v)
        ))
    )
    gain_load.start()
    for a in range(2):
        for c in (low_loads[a], high_loads[a], loads[a]):
            c.start()

    early = raw * step
    outs = (out_g, out_u)
    every = [(a, k) for a in range(2) for k in range(chunks)]
    started = {}

    def move(slot, a, k, owner, target, base=None):
        r = pl.ds(pl.multiple_of(owner * rows + k * step, 16), step)
        part = outs[a].at[r, :]
        return pltpu.make_async_remote_copy(
            src_ref=part if base is None else base.at[k * step:(k + 1) * step, :],
            dst_ref=part,
            send_sem=send.at[slot, a * chunks + k], recv_sem=recv.at[slot, a * chunks + k],
            device_id={AXIS: target})

    def go(*args):
        started[args[:3]] = move(*args)
        started[args[:3]].start()

    def send_own(a, k):
        go(0, a, k, me, to_x)
        go(1, a, k, me, to_y)
        go(2, a, k, me, sib)

    def send_raw(a, k):
        go(0, a, k, me, to_x, wg_hbm)
        go(1, a, k, me, to_y, wg_hbm)
        go(2, a, k, me, sib, wg_hbm)

    pl.semaphore_wait(barrier, n - 1)
    send_raw(0, 0)

    gain_load.wait()
    col_v[...] = jnp.broadcast_to(gain_v[...], (128, rows)).T
    for a in range(2):
        low_loads[a].wait()
        low_v[a] = (mix_rate * l_v[a].astype(jnp.float32)).T.astype(jnp.bfloat16)
        high_loads[a].wait()
        loads[a].wait()
        acc = jnp.zeros((8, cols), jnp.float32)
        for k in range(chunks):
            r = pl.ds(k * step, step)
            prod = jnp.dot(low_v[a, r, :], h_v[a], preferred_element_type=jnp.float32)
            new = (w_v[a, r, :].astype(jnp.float32) + prod) * col_v[r, 0:1]
            g_v[a, r, :] = new
            acc = acc + jnp.sum((new * new).reshape(step // 8, 8, cols), axis=0)
        sums[me, :, a * cols:(a + 1) * cols] = jnp.sum(acc, axis=0, keepdims=True)

    sums[me, :, 2 * cols:] = gain_v[:, :early]
    shares = []
    for d in range(1, n):
        shares.append(pltpu.make_async_remote_copy(
            src_ref=sums.at[me], dst_ref=sums.at[me],
            send_sem=ssum.at[d], recv_sem=rsum.at[d],
            device_id={AXIS: lax.rem(me + d, n)}))
        shares[-1].start()
    lows = []
    for d in range(1, n):
        lows.append(pltpu.make_async_remote_copy(
            src_ref=l_v.at[0, :, :early], dst_ref=far_low.at[me],
            send_sem=slow.at[d], recv_sem=rlow.at[d],
            device_id={AXIS: lax.rem(me + d, n)}))
        lows[-1].start()
    for k in range(1, raw):
        send_raw(0, k)
    for c in shares:
        c.wait_recv()
    total = sums[0, :, :2 * cols]
    for d in range(1, n):
        total = total + sums[d, :, :2 * cols]
    factor = jnp.sqrt(total)
    fac[...] = factor
    rf_v[...] = 1.0 / factor

    for i, (a, k) in enumerate(every):
        new = g_v[a, k * step:(k + 1) * step, :] * rf_v[:, a * cols:(a + 1) * cols]
        r = pl.ds(pl.multiple_of(me * rows + k * step, 16), step)
        outs[a][r, :] = new.astype(jnp.bfloat16)
        if i > raw:
            send_own(*every[i - 1])
    send_own(*every[-1])

    for i, (a, k) in enumerate(every):
        move(0, a, k, to_x, to_x).wait_recv()
        if i % 2 == 0:
            go(5, a, k, to_x, to_y)
        go(3, a, k, to_x, sib)
        move(1, a, k, to_y, to_y).wait_recv()
        if i % 2 == 1:
            go(5, a, k, to_y, to_x)
        go(4, a, k, to_y, sib)

    flip = 1 - 2 * core

    def from_sib(a, k):
        move(2, a, k, sib, sib).wait_recv()
        move(3, a, k, to_x + flip, sib).wait_recv()
        move(4, a, k, to_y + flip, sib).wait_recv()
        move(6, a, k, diag + flip, sib).wait_recv()

    def finish_raw():
        for a, k in every[:raw]:
            from_sib(a, k)
            for slot in (3, 4, 5, 6):
                started.pop((slot, a, k)).wait_send()
        for c in lows:
            c.wait_recv()

        @pl.loop(1, n)
        def _(d):
            owner = lax.rem(me + d, n)
            low = (mix_rate * far_low[owner].astype(jnp.float32)).T.astype(jnp.bfloat16)
            col = jnp.broadcast_to(sums[owner, :, 2 * cols:], (128, early)).T[:, 0:1]
            r = pl.ds(pl.multiple_of(owner * rows, 16), early)
            prod = jnp.dot(low, h_v[0], preferred_element_type=jnp.float32)
            new = (out_g[r, :].astype(jnp.float32) + prod) * col
            out_g[r, :] = (new * rf_v[:, :cols]).astype(jnp.bfloat16)

    for i, (a, k) in enumerate(every):
        if i == 3 * raw:
            finish_raw()
        move(5, a, k, diag, to_x).wait_recv()
        go(6, a, k, diag, sib)
    for a, k in every[raw:]:
        from_sib(a, k)
    for c in started.values():
        c.wait_send()
    for c in shares + lows:
        c.wait_send()


def write_kernel(parts, a_v, b_v, fac, a_hbm, b_hbm, fa_hbm, fb_hbm, sem, fac_sem):
    rows, cols = a_v.shape
    step = rows // parts
    copies = [
        pltpu.make_async_copy(fac.at[0, i * cols:(i + 1) * cols], dst, fac_sem.at[i])
        for i, dst in enumerate((fa_hbm, fb_hbm))
    ]
    for i, (src, dst) in enumerate(((a_v, a_hbm), (b_v, b_hbm))):
        for k in range(parts):
            r = pl.ds(k * step, step)
            copies.append(pltpu.make_async_copy(src.at[r, :], dst.at[r, :], sem.at[i, k]))
    for c in copies:
        c.start()
    for c in copies:
        c.wait()


def paired(n, weight_gate, low_gate, high_gate, weight_up, low_up, high_up, norm_gain):
    rows, cols = weight_gate.shape
    chunks, raw = 5, 2
    early = raw * rows // chunks
    full = (n * rows, cols)
    vmem = pl.BlockSpec(memory_space=pltpu.VMEM)
    hbm = pl.BlockSpec(memory_space=pl.ANY)
    space = pl.BlockSpec(memory_space=pltpu.HBM)
    rank = high_gate.shape[0]
    grant = 65472 * 2**10 - (4 * full[0] * cols + 8 * cols) // 2**10 * 2**10 - 24 * 2**10
    gate, up, fac = pl.pallas_call(
        functools.partial(gather_kernel, n, chunks, raw),
        out_shape=(
            pltpu.VMEM(full, jnp.bfloat16),
            pltpu.VMEM(full, jnp.bfloat16),
            pltpu.VMEM((1, 2 * cols), jnp.float32),
        ),
        in_specs=[space] * 7,
        out_specs=(vmem, vmem, vmem),
        scratch_shapes=[
            pltpu.VMEM((2, rows, cols), jnp.bfloat16),
            pltpu.VMEM((2, rank, rows), jnp.bfloat16),
            pltpu.VMEM((2, rank, cols), jnp.bfloat16),
            pltpu.VMEM((1, rows), jnp.float32),
            pltpu.VMEM((2, rows, rank), jnp.bfloat16),
            pltpu.VMEM((2, rows, cols), jnp.float32),
            pltpu.VMEM((rows, 128), jnp.float32),
            pltpu.VMEM((n, 1, 2 * cols + early), jnp.float32),
            pltpu.VMEM((1, 2 * cols), jnp.float32),
            pltpu.VMEM((n, rank, early), jnp.bfloat16),
            pltpu.SemaphoreType.DMA((7,)),
            pltpu.SemaphoreType.DMA((n,)),
            pltpu.SemaphoreType.DMA((n,)),
            pltpu.SemaphoreType.DMA((n,)),
            pltpu.SemaphoreType.DMA((n,)),
            pltpu.SemaphoreType.DMA((7, 2 * chunks)),
            pltpu.SemaphoreType.DMA((7, 2 * chunks)),
        ],
        compiler_params=pltpu.CompilerParams(
            collective_id=0, has_side_effects=True, vmem_limit_bytes=grant
        ),
        name="merge_gather",
    )(weight_gate, weight_up, low_gate.T, low_up.T, high_gate, high_up, norm_gain)
    parts = 8
    return pl.pallas_call(
        functools.partial(write_kernel, parts),
        out_shape=(jax.ShapeDtypeStruct(full, jnp.bfloat16),) * 2
        + (jax.ShapeDtypeStruct((cols,), jnp.float32),) * 2,
        in_specs=[vmem, vmem, vmem],
        out_specs=(hbm,) * 4,
        scratch_shapes=[pltpu.SemaphoreType.DMA((2, parts)), pltpu.SemaphoreType.DMA((2,))],
        compiler_params=pltpu.CompilerParams(vmem_limit_bytes=2**20),
        name="write_out",
    )(gate, up, fac)


def solution(mesh):
    in_specs = (
        P("shard", "tp"),
        P("shard", None),
        P(None, "tp"),
        P("shard", "tp"),
        P("shard", None),
        P(None, "tp"),
        P("shard"),
    )
    out_specs = (P(None, "tp"), P(None, "tp"), P("tp"), P("tp"))
    n = mesh.shape[AXIS]
    side = math.isqrt(n // 2)
    body = functools.partial(paired, n) if side == 2 and 2 * side * side == n else local
    return jax.shard_map(body, mesh=mesh, in_specs=in_specs, out_specs=out_specs, check_vma=False)
```

```python
import functools
import math

import jax
import jax.numpy as jnp
from jax import lax
from jax.experimental import pallas as pl
from jax.experimental.pallas import tpu as pltpu
from jax.sharding import PartitionSpec as P

mix_rate = 2.0
AXIS = "shard"


def local(weight_gate, low_gate, high_gate, weight_up, low_up, high_up, norm_gain):
    latest_gate = weight_gate.astype(jnp.float32) + mix_rate * jnp.dot(
        low_gate, high_gate, preferred_element_type=jnp.float32
    )
    latest_up = weight_up.astype(jnp.float32) + mix_rate * jnp.dot(
        low_up, high_up, preferred_element_type=jnp.float32
    )
    latest_gained_gate = latest_gate * norm_gain[:, None]
    latest_gained_up = latest_up * norm_gain[:, None]
    total_gate, total_up = lax.psum(
        (
            jnp.sum(latest_gained_gate * latest_gained_gate, axis=0),
            jnp.sum(latest_gained_up * latest_gained_up, axis=0),
        ),
        AXIS,
    )
    factor_gate = jnp.sqrt(total_gate)
    factor_up = jnp.sqrt(total_up)
    narrow_gate = (latest_gained_gate / factor_gate).astype(jnp.bfloat16)
    narrow_up = (latest_gained_up / factor_up).astype(jnp.bfloat16)
    ready_gate = lax.all_gather(narrow_gate, AXIS, axis=0, tiled=True)
    ready_up = lax.all_gather(narrow_up, AXIS, axis=0, tiled=True)
    return (ready_gate, ready_up, factor_gate, factor_up)


late = 0


def place():
    me = lax.axis_index(AXIS)
    core = lax.rem(me, 2)
    x = lax.rem(me // 2, 2)
    y = me // 4
    to_x = me + 2 - 4 * x
    to_y = me + 4 - 8 * y
    return me, core, me + 1 - 2 * core, to_x, to_y, to_x + 4 - 8 * y, 1 - 2 * core


def pairs(start, *sizes):
    out = []
    for z in sizes:
        for _ in range(2):
            out.append((start, z))
            start += z
    return out


def gather_kernel(
    unit, solo, wg_hbm, wu_hbm, lg_hbm, lu_hbm, hg_hbm, hu_hbm, gain_hbm,
    out_g, out_u, fac,
    w_v, l_v, h_v, gain_v, low_v, g_v, col_v, part, mine, heard, rf_v,
    raw_v, far_l, far_g, far_low, far_col,
    in_sem, small_send, small_recv, send, recv,
):
    rows, cols = wg_hbm.shape
    me, core, sib, to_x, to_y, diag, flip = place()
    early = 4 * unit
    shared_up = rows - solo
    raws = [(0, s, z) for s, z in pairs(0, unit, unit)]
    bulk = [(0, s, z) for s, z in pairs(early, 3 * unit)]
    bulk += [(1, s, z) for s, z in (
        pairs(0, 2 * unit, unit) if solo else pairs(0, 3 * unit, unit, unit))]
    alone = [(1, s, z) for s, z in pairs(shared_up, unit, unit)] if solo else []
    block = (0, 0, early)
    every = raws + bulk
    order = {c: i for i, c in enumerate(every + alone + [block])}
    outs = (out_g, out_u)

    barrier = pltpu.get_barrier_semaphore()
    for d in (to_x, to_y, sib):
        pl.semaphore_signal(barrier, inc=1, device_id={AXIS: d})

    gain_load = pltpu.make_async_copy(gain_hbm, gain_v.at[0], in_sem.at[6])
    low_loads, high_loads, loads = (
        [
            pltpu.make_async_copy(src, dst.at[a], in_sem.at[3 * a + i])
            for a, src in enumerate(pair)
        ]
        for i, (pair, dst) in enumerate((
            ((lg_hbm, lu_hbm), l_v), ((hg_hbm, hu_hbm), h_v), ((wg_hbm, wu_hbm), w_v)
        ))
    )
    gain_load.start()
    for a in range(2):
        for c in (low_loads[a], high_loads[a], loads[a]):
            c.start()

    started = []

    def keep(c):
        started.append(c)
        c.start()

    def remote(src, dst, slot, chunk, target):
        i = order[chunk]
        return pltpu.make_async_remote_copy(
            src_ref=src, dst_ref=dst, send_sem=send.at[slot, i],
            recv_sem=recv.at[slot, i], device_id={AXIS: target})

    def small(src, dst, i, target):
        return pltpu.make_async_remote_copy(
            src_ref=src, dst_ref=dst, send_sem=small_send.at[i],
            recv_sem=small_recv.at[i], device_id={AXIS: target})

    def piece(chunk, owner):
        a, s, z = chunk
        return outs[a].at[pl.ds(pl.multiple_of(owner * rows + s, 16), z), :]

    def move(slot, chunk, owner, target):
        p = piece(chunk, owner)
        return remote(p, p, slot, chunk, target)

    def raw_move(slot, chunk, at, target):
        _, s, z = chunk
        src = wg_hbm.at[s:s + z, :] if slot < 2 else raw_v.at[at, s:s + z, :]
        return remote(src, raw_v.at[slot if slot < 2 else 2, s:s + z, :], slot, chunk, target)

    def send_raw(chunk, x_only=None):
        if x_only is not False:
            keep(raw_move(0, chunk, 0, to_x))
        if x_only is not True:
            keep(raw_move(1, chunk, 0, to_y))

    pl.semaphore_wait(barrier, 3)
    send_raw(raws[0])
    send_raw(raws[1])

    gain_load.wait()
    col_v[...] = jnp.broadcast_to(gain_v[...], (128, rows)).T
    step = 2 * unit
    for a in range(2):
        low_loads[a].wait()
        low_v[a] = (mix_rate * l_v[a].astype(jnp.float32)).T.astype(jnp.bfloat16)
        high_loads[a].wait()
        loads[a].wait()
        acc = jnp.zeros((8, cols), jnp.float32)
        for s in range(0, rows, step):
            r = pl.ds(s, step)
            prod = jnp.dot(low_v[a, r, :], h_v[a], preferred_element_type=jnp.float32)
            new = (w_v[a, r, :].astype(jnp.float32) + prod) * col_v[r, 0:1]
            g_v[a, r, :] = new
            acc = acc + jnp.sum((new * new).reshape(step // 8, 8, cols), axis=0)
        part[a] = jnp.sum(acc, axis=0, keepdims=True)

    keep(small(part.at[1 - core], heard.at[0], 0, sib))
    low_own, gain_own = l_v.at[0, :, :early], gain_v.at[:, :early]
    for i, d in enumerate((to_x, to_y)):
        keep(small(low_own, far_l.at[i], 4 + i, d))
        keep(small(gain_own, far_g.at[i], 7 + i, d))
    small(part.at[0], heard.at[0], 0, sib).wait_recv()
    mine[0] = part[core] + heard[0]
    send_raw(raws[2], False)
    keep(small(mine.at[0], heard.at[1], 1, to_x))
    send_raw(raws[2], True)
    small(mine.at[0], heard.at[1], 1, to_x).wait_recv()
    mine[1] = mine[0] + heard[1]
    send_raw(raws[3], True)
    keep(small(mine.at[1], heard.at[2], 2, to_y))
    send_raw(raws[3], False)
    small(mine.at[1], heard.at[2], 2, to_y).wait_recv()
    mine[2 + core] = mine[1] + heard[2]
    keep(small(mine.at[2 + core], mine.at[2 + core], 3, sib))
    small(mine.at[2], mine.at[2], 3, sib).wait_recv()
    for a in range(2):
        factor = jnp.sqrt(mine[2 + a])
        fac[a] = factor
        rf_v[a] = 1.0 / factor

    def scale(chunk):
        a, s, z = chunk
        r = pl.ds(pl.multiple_of(me * rows + s, 16), z)
        outs[a][r, :] = (g_v[a, s:s + z, :] * rf_v[a]).astype(jnp.bfloat16)

    def send_own(chunk):
        keep(move(0, chunk, me, to_x))
        keep(move(1, chunk, me, to_y))
        keep(move(2, chunk, me, sib))

    for i, chunk in enumerate(bulk):
        scale(chunk)
        if i:
            send_own(bulk[i - 1])
    scale(block)
    send_own(bulk[-1])
    for chunk in alone:
        scale(chunk)
    keep(move(2, block, me, sib))

    low_x, low_y = (small(low_own, far_l.at[i], 4 + i, to_x) for i in range(2))
    gain_x, gain_y = (small(gain_own, far_g.at[i], 7 + i, to_x) for i in range(2))
    low_x.wait_recv()
    keep(small(far_l.at[0], far_l.at[2], 6, to_y))
    gain_x.wait_recv()
    keep(small(far_g.at[0], far_g.at[2], 9, to_y))
    low_y.wait_recv()
    gain_y.wait_recv()

    def correct(i, owner):
        far_low[i] = (mix_rate * far_l[i].astype(jnp.float32)).T.astype(jnp.bfloat16)
        far_col[i] = jnp.broadcast_to(far_g[i], (128, early)).T
        for s in range(0, early, step):
            r = pl.ds(s, step)
            prod = jnp.dot(far_low[i, r, :], h_v[0], preferred_element_type=jnp.float32)
            new = (raw_v[i, r, :].astype(jnp.float32) + prod) * far_col[i, r, 0:1]
            o = pl.ds(pl.multiple_of(owner * rows + s, 16), step)
            out_g[o, :] = (new * rf_v[0]).astype(jnp.bfloat16)

    for i, chunk in enumerate(raws):
        raw_move(0, chunk, 0, to_x).wait_recv()
        if i % 2 == 0:
            keep(raw_move(5, chunk, 0, to_y))
        raw_move(1, chunk, 0, to_y).wait_recv()
        if i % 2 == 1:
            keep(raw_move(5, chunk, 1, to_x))
    correct(0, to_x)
    correct(1, to_y)

    def relay(i, chunk, keep, forward):
        move(0, chunk, to_x, to_x).wait_recv()
        if i % 2 == 0:
            keep(move(5, chunk, to_x, to_y))
        if forward:
            keep(move(3, chunk, to_x, sib))
        move(1, chunk, to_y, to_y).wait_recv()
        if i % 2 == 1:
            keep(move(5, chunk, to_y, to_x))
        if forward:
            keep(move(4, chunk, to_y, sib))

    for i, chunk in enumerate(bulk):
        relay(i, chunk, keep, True)
        if i == 0:
            keep(move(3, block, to_x, sib))
            keep(move(4, block, to_y, sib))

    if solo:
        @pl.when(core == late)
        def _():
            for chunk in alone:
                move(0, chunk, me, to_x).start()
                move(1, chunk, me, to_y).start()

    for chunk in raws:
        raw_move(5, chunk, 0, to_x).wait_recv()
    small(far_l.at[0], far_l.at[2], 6, to_y).wait_recv()
    small(far_g.at[0], far_g.at[2], 9, to_y).wait_recv()
    correct(2, diag)
    for i, chunk in enumerate(bulk):
        move(5, chunk, diag, to_x).wait_recv()
        keep(move(6, chunk, diag, sib))
        if i == 0:
            keep(move(6, block, diag, sib))
    for chunk in [block] + bulk:
        move(2, chunk, sib, sib).wait_recv()
        move(3, chunk, to_x + flip, sib).wait_recv()
        move(4, chunk, to_y + flip, sib).wait_recv()
        move(6, chunk, diag + flip, sib).wait_recv()

    if solo:
        @pl.when(core == late)
        def _():
            own = []

            def go(c):
                own.append(c)
                c.start()

            for i, chunk in enumerate(alone):
                relay(i, chunk, go, False)
            for chunk in alone:
                move(5, chunk, diag, to_x).wait_recv()
                move(0, chunk, me, to_x).wait_send()
                move(1, chunk, me, to_y).wait_send()
            for c in own:
                c.wait_send()

    for c in started:
        c.wait_send()


def tail_kernel(rows, unit, up, after, tail, ready, send, recv):
    solo = tail.shape[1]
    me, core, sib, to_x, to_y, diag, flip = place()
    chunks = pairs(0, unit, unit)
    whole = (0, solo)
    lines = len(chunks)
    barrier = pltpu.get_barrier_semaphore()

    def remote(src, dst, slot, i, target):
        return pltpu.make_async_remote_copy(
            src_ref=src, dst_ref=dst, send_sem=send.at[slot, i],
            recv_sem=recv.at[slot, i], device_id={AXIS: target})

    def held(owner, s, z):
        return up.at[pl.ds(pl.multiple_of(owner * rows + rows - solo + s, 16), z), :]

    def move(slot, i, chunk, owner, target, first=False):
        s, z = chunk
        dst = tail.at[owner, s:s + z, :]
        return remote(held(owner, s, z) if first else dst, dst, slot, i, target)

    def copy(owner):
        r = pl.ds(pl.multiple_of(owner * rows + rows - solo, 16), solo)
        tail[owner] = up[r, :]

    @pl.when(core != late)
    def _():
        started = []

        def keep(c):
            started.append(c)
            c.start()

        for d in (to_x, to_y, sib):
            pl.semaphore_signal(barrier, inc=1, device_id={AXIS: d})
        pl.semaphore_wait(barrier, 2)
        for i, c in enumerate(chunks):
            keep(move(0, i, c, me, to_x, True))
            keep(move(1, i, c, me, to_y, True))
        copy(me)
        for i, c in enumerate(chunks):
            move(0, i, c, to_x, to_x).wait_recv()
            if i % 2 == 0:
                keep(move(5, i, c, to_x, to_y))
            move(1, i, c, to_y, to_y).wait_recv()
            if i % 2 == 1:
                keep(move(5, i, c, to_y, to_x))
        pl.semaphore_wait(ready, 1)
        keep(move(2, 0, whole, me, sib, True))
        keep(move(3, 0, whole, to_x, sib))
        keep(move(4, 0, whole, to_y, sib))
        for i, c in enumerate(chunks):
            move(5, i, c, diag, to_x).wait_recv()
            keep(move(6, i, c, diag, sib))
        for i in range(4):
            move(7, i, whole, 2 * i + late, sib).wait_recv()
        for c in started:
            c.wait_send()

    @pl.when(core == late)
    def _():
        pl.semaphore_wait(barrier, 1)
        pl.semaphore_signal(ready, inc=1, device_id={AXIS: sib})
        out = [move(7, i, whole, 2 * i + late, sib, True) for i in range(4)]
        for c in out:
            c.start()
        for i in range(4):
            copy(2 * i + late)
        move(2, 0, whole, sib, sib).wait_recv()
        move(3, 0, whole, to_x + flip, sib).wait_recv()
        move(4, 0, whole, to_y + flip, sib).wait_recv()
        for i, c in enumerate(chunks):
            move(6, i, c, diag + flip, sib).wait_recv()
        for c in out:
            c.wait_send()


def write_kernel(rows, solo, a_v, b_v, fac, a_hbm, b_hbm, fa_hbm, fb_hbm, done, sem, fac_sem):
    done[...] = jnp.zeros_like(done)
    n = a_v.shape[0] // rows
    copies = [
        pltpu.make_async_copy(fac.at[i, 0], dst, fac_sem.at[i])
        for i, dst in enumerate((fa_hbm, fb_hbm))
    ]
    for i, (src, dst, z) in enumerate(((a_v, a_hbm, rows), (b_v, b_hbm, rows - solo))):
        for k in range(n):
            r = pl.ds(k * rows, z)
            copies.append(pltpu.make_async_copy(src.at[r, :], dst.at[r, :], sem.at[i, k]))
    for c in copies:
        c.start()
    for c in copies:
        c.wait()


def finish_kernel(rows, tail, before, b_hbm, sem):
    n, solo, _ = tail.shape
    copies = [
        pltpu.make_async_copy(
            tail.at[k], b_hbm.at[pl.ds((k + 1) * rows - solo, solo), :], sem.at[k])
        for k in range(n)
    ]
    for c in copies:
        c.start()
    for c in copies:
        c.wait()


def paired(n, weight_gate, low_gate, high_gate, weight_up, low_up, high_up, norm_gain):
    rows, cols = weight_gate.shape
    unit = rows // 10
    solo = 4 * unit
    early = 4 * unit
    full = (n * rows, cols)
    vmem = pl.BlockSpec(memory_space=pltpu.VMEM)
    hbm = pl.BlockSpec(memory_space=pl.ANY)
    space = pl.BlockSpec(memory_space=pltpu.HBM)
    rank = high_gate.shape[0]
    grant = 65472 * 2**10 - (4 * full[0] * cols + 8 * cols) // 2**10 * 2**10 - 24 * 2**10
    slots = 20
    gate, up, fac = pl.pallas_call(
        functools.partial(gather_kernel, unit, solo),
        out_shape=(
            pltpu.VMEM(full, jnp.bfloat16),
            pltpu.VMEM(full, jnp.bfloat16),
            pltpu.VMEM((2, 1, cols), jnp.float32),
        ),
        in_specs=[space] * 7,
        out_specs=(vmem, vmem, vmem),
        scratch_shapes=[
            pltpu.VMEM((2, rows, cols), jnp.bfloat16),
            pltpu.VMEM((2, rank, rows), jnp.bfloat16),
            pltpu.VMEM((2, rank, cols), jnp.bfloat16),
            pltpu.VMEM((1, rows), jnp.float32),
            pltpu.VMEM((2, rows, rank), jnp.bfloat16),
            pltpu.VMEM((2, rows, cols), jnp.float32),
            pltpu.VMEM((rows, 128), jnp.float32),
            pltpu.VMEM((2, 1, cols), jnp.float32),
            pltpu.VMEM((4, 1, cols), jnp.float32),
            pltpu.VMEM((3, 1, cols), jnp.float32),
            pltpu.VMEM((2, 1, cols), jnp.float32),
            pltpu.VMEM((3, early, cols), jnp.bfloat16),
            pltpu.VMEM((3, rank, early), jnp.bfloat16),
            pltpu.VMEM((3, 1, early), jnp.float32),
            pltpu.VMEM((3, early, rank), jnp.bfloat16),
            pltpu.VMEM((3, early, 128), jnp.float32),
            pltpu.SemaphoreType.DMA((7,)),
            pltpu.SemaphoreType.DMA((10,)),
            pltpu.SemaphoreType.DMA((10,)),
            pltpu.SemaphoreType.DMA((7, slots)),
            pltpu.SemaphoreType.DMA((7, slots)),
        ],
        compiler_params=pltpu.CompilerParams(
            collective_id=0, has_side_effects=True, vmem_limit_bytes=grant
        ),
        name="merge_gather",
    )(weight_gate, weight_up, low_gate.T, low_up.T, high_gate, high_up, norm_gain)
    whole = jax.ShapeDtypeStruct(full, jnp.bfloat16)
    ready_gate, ready_up, factor_gate, factor_up, done = pl.pallas_call(
        functools.partial(write_kernel, rows, solo),
        out_shape=(whole, whole) + (jax.ShapeDtypeStruct((cols,), jnp.float32),) * 2
        + (pltpu.VMEM((8, 128), jnp.float32),),
        in_specs=[vmem, vmem, vmem],
        out_specs=(hbm,) * 4 + (vmem,),
        scratch_shapes=[pltpu.SemaphoreType.DMA((2, n)), pltpu.SemaphoreType.DMA((2,))],
        compiler_params=pltpu.CompilerParams(vmem_limit_bytes=2**20),
        name="write_out",
    )(gate, up, fac)
    if solo:
        tail = pl.pallas_call(
            functools.partial(tail_kernel, rows, unit),
            out_shape=pltpu.VMEM((n, solo, cols), jnp.bfloat16),
            in_specs=[vmem, vmem],
            out_specs=vmem,
            scratch_shapes=[
                pltpu.SemaphoreType.REGULAR,
                pltpu.SemaphoreType.DMA((8, 4)),
                pltpu.SemaphoreType.DMA((8, 4)),
            ],
            compiler_params=pltpu.CompilerParams(
                collective_id=1, has_side_effects=True, vmem_limit_bytes=2**20
            ),
            name="tail_gather",
        )(up, done)
        ready_up = pl.pallas_call(
            functools.partial(finish_kernel, rows),
            out_shape=whole,
            in_specs=[vmem, hbm],
            out_specs=hbm,
            input_output_aliases={1: 0},
            scratch_shapes=[pltpu.SemaphoreType.DMA((n,))],
            compiler_params=pltpu.CompilerParams(vmem_limit_bytes=2**20),
            name="finish",
        )(tail, ready_up)
    return ready_gate, ready_up, factor_gate, factor_up


def solution(mesh):
    in_specs = (
        P("shard", "tp"),
        P("shard", None),
        P(None, "tp"),
        P("shard", "tp"),
        P("shard", None),
        P(None, "tp"),
        P("shard"),
    )
    out_specs = (P(None, "tp"), P(None, "tp"), P("tp"), P("tp"))
    n = mesh.shape[AXIS]
    side = math.isqrt(n // 2)
    body = functools.partial(paired, n) if side == 2 and 2 * side * side == n else local
    return jax.shard_map(body, mesh=mesh, in_specs=in_specs, out_specs=out_specs, check_vma=False)
```

```python
import functools
import math

import jax
import jax.numpy as jnp
from jax import lax
from jax.experimental import pallas as pl
from jax.experimental.pallas import tpu as pltpu
from jax.sharding import PartitionSpec as P

mix_rate = 2.0
AXIS = "shard"


def local(weight_gate, low_gate, high_gate, weight_up, low_up, high_up, norm_gain):
    latest_gate = weight_gate.astype(jnp.float32) + mix_rate * jnp.dot(
        low_gate, high_gate, preferred_element_type=jnp.float32
    )
    latest_up = weight_up.astype(jnp.float32) + mix_rate * jnp.dot(
        low_up, high_up, preferred_element_type=jnp.float32
    )
    latest_gained_gate = latest_gate * norm_gain[:, None]
    latest_gained_up = latest_up * norm_gain[:, None]
    total_gate, total_up = lax.psum(
        (
            jnp.sum(latest_gained_gate * latest_gained_gate, axis=0),
            jnp.sum(latest_gained_up * latest_gained_up, axis=0),
        ),
        AXIS,
    )
    factor_gate = jnp.sqrt(total_gate)
    factor_up = jnp.sqrt(total_up)
    narrow_gate = (latest_gained_gate / factor_gate).astype(jnp.bfloat16)
    narrow_up = (latest_gained_up / factor_up).astype(jnp.bfloat16)
    ready_gate = lax.all_gather(narrow_gate, AXIS, axis=0, tiled=True)
    ready_up = lax.all_gather(narrow_up, AXIS, axis=0, tiled=True)
    return (ready_gate, ready_up, factor_gate, factor_up)


late = 0
RAW = (4, 4)
GATE = (12,)
UP = (4, 4)
ALONE = (8, 4)


def place():
    me = lax.axis_index(AXIS)
    core = lax.rem(me, 2)
    x = lax.rem(me // 2, 2)
    y = me // 4
    to_x = me + 2 - 4 * x
    to_y = me + 4 - 8 * y
    return me, core, me + 1 - 2 * core, to_x, to_y, to_x + 4 - 8 * y, 1 - 2 * core


def pairs(start, unit, sizes):
    out = []
    for z in sizes:
        for _ in range(2):
            out.append((start, z * unit))
            start += z * unit
    return out


def gather_kernel(
    unit, solo, wg_hbm, wu_hbm, lg_hbm, lu_hbm, hg_hbm, hu_hbm, gain_hbm,
    out_g, out_u, fac,
    w_v, l_v, h_v, gain_v, low_v, g_v, col_v, part, mine, heard, rf_v,
    raw_v, far_l, far_g, far_low, far_col,
    in_sem, small_send, small_recv, send, recv,
):
    rows, cols = wg_hbm.shape
    me, core, sib, to_x, to_y, diag, flip = place()
    early = 2 * sum(RAW) * unit
    shared_up = rows - solo
    raws = [(0, s, z) for s, z in pairs(0, unit, RAW)]
    bulk = [(0, s, z) for s, z in pairs(early, unit, GATE)]
    bulk += [(1, s, z) for s, z in pairs(0, unit, UP)]
    alone = [(1, s, z) for s, z in pairs(shared_up, unit, ALONE)]
    own_tail = (1, shared_up, solo)
    block = (0, 0, early)
    every = raws + bulk
    order = {c: i for i, c in enumerate(every + alone + [block, own_tail])}
    outs = (out_g, out_u)

    barrier = pltpu.get_barrier_semaphore()
    for d in (to_x, to_y, sib):
        pl.semaphore_signal(barrier, inc=1, device_id={AXIS: d})

    gain_load = pltpu.make_async_copy(gain_hbm, gain_v.at[0], in_sem.at[6])
    low_loads, high_loads, loads = (
        [
            pltpu.make_async_copy(src, dst.at[a], in_sem.at[3 * a + i])
            for a, src in enumerate(pair)
        ]
        for i, (pair, dst) in enumerate((
            ((lg_hbm, lu_hbm), l_v), ((hg_hbm, hu_hbm), h_v), ((wg_hbm, wu_hbm), w_v)
        ))
    )
    gain_load.start()
    for a in range(2):
        for c in (low_loads[a], high_loads[a], loads[a]):
            c.start()

    started = []

    def keep(c):
        started.append(c)
        c.start()

    def remote(src, dst, slot, chunk, target):
        i = order[chunk]
        return pltpu.make_async_remote_copy(
            src_ref=src, dst_ref=dst, send_sem=send.at[slot, i],
            recv_sem=recv.at[slot, i], device_id={AXIS: target})

    def small(src, dst, i, target):
        return pltpu.make_async_remote_copy(
            src_ref=src, dst_ref=dst, send_sem=small_send.at[i],
            recv_sem=small_recv.at[i], device_id={AXIS: target})

    def piece(chunk, owner):
        a, s, z = chunk
        return outs[a].at[pl.ds(pl.multiple_of(owner * rows + s, 8), z), :]

    def move(slot, chunk, owner, target):
        p = piece(chunk, owner)
        return remote(p, p, slot, chunk, target)

    def raw_move(slot, chunk, at, target):
        _, s, z = chunk
        src = wg_hbm.at[s:s + z, :] if slot < 2 else raw_v.at[at, s:s + z, :]
        return remote(src, raw_v.at[slot if slot < 2 else 2, s:s + z, :], slot, chunk, target)

    def send_raw(chunk, x_only=None):
        if x_only is not False:
            keep(raw_move(0, chunk, 0, to_x))
        if x_only is not True:
            keep(raw_move(1, chunk, 0, to_y))

    pl.semaphore_wait(barrier, 3)
    send_raw(raws[0])
    send_raw(raws[1])

    gain_load.wait()
    col_v[...] = jnp.broadcast_to(gain_v[...], (128, rows)).T
    step = rows // 5
    for a in range(2):
        low_loads[a].wait()
        low_v[a] = (mix_rate * l_v[a].astype(jnp.float32)).T.astype(jnp.bfloat16)
        high_loads[a].wait()
        loads[a].wait()
        acc = jnp.zeros((8, cols), jnp.float32)
        for s in range(0, rows, step):
            r = pl.ds(s, step)
            prod = jnp.dot(low_v[a, r, :], h_v[a], preferred_element_type=jnp.float32)
            new = (w_v[a, r, :].astype(jnp.float32) + prod) * col_v[r, 0:1]
            g_v[a, r, :] = new
            acc = acc + jnp.sum((new * new).reshape(step // 8, 8, cols), axis=0)
        part[a] = jnp.sum(acc, axis=0, keepdims=True)

    keep(small(part.at[1 - core], heard.at[0], 0, sib))
    low_own, gain_own = l_v.at[0, :, :early], gain_v.at[:, :early]
    for i, d in enumerate((to_x, to_y)):
        keep(small(low_own, far_l.at[i], 4 + i, d))
        keep(small(gain_own, far_g.at[i], 7 + i, d))
    small(part.at[0], heard.at[0], 0, sib).wait_recv()
    mine[0] = part[core] + heard[0]
    send_raw(raws[2], False)
    keep(small(mine.at[0], heard.at[1], 1, to_x))
    send_raw(raws[2], True)
    small(mine.at[0], heard.at[1], 1, to_x).wait_recv()
    mine[1] = mine[0] + heard[1]
    send_raw(raws[3], True)
    keep(small(mine.at[1], heard.at[2], 2, to_y))
    send_raw(raws[3], False)
    small(mine.at[1], heard.at[2], 2, to_y).wait_recv()
    mine[2 + core] = mine[1] + heard[2]
    keep(small(mine.at[2 + core], mine.at[2 + core], 3, sib))
    small(mine.at[2], mine.at[2], 3, sib).wait_recv()
    for a in range(2):
        factor = jnp.sqrt(mine[2 + a])
        fac[a] = factor
        rf_v[a] = 1.0 / factor

    def scale(chunk):
        a, s, z = chunk
        r = pl.ds(pl.multiple_of(me * rows + s, 8), z)
        outs[a][r, :] = (g_v[a, s:s + z, :] * rf_v[a]).astype(jnp.bfloat16)

    def send_own(chunk):
        keep(move(0, chunk, me, to_x))
        keep(move(1, chunk, me, to_y))
        keep(move(2, chunk, me, sib))

    for i, chunk in enumerate(bulk):
        scale(chunk)
        if i:
            send_own(bulk[i - 1])
    scale(block)
    send_own(bulk[-1])
    for chunk in alone:
        scale(chunk)
    keep(move(2, block, me, sib))
    keep(move(2, own_tail, me, sib))

    low_x, low_y = (small(low_own, far_l.at[i], 4 + i, to_x) for i in range(2))
    gain_x, gain_y = (small(gain_own, far_g.at[i], 7 + i, to_x) for i in range(2))
    low_x.wait_recv()
    keep(small(far_l.at[0], far_l.at[2], 6, to_y))
    gain_x.wait_recv()
    keep(small(far_g.at[0], far_g.at[2], 9, to_y))
    low_y.wait_recv()
    gain_y.wait_recv()

    def correct(i, owner):
        far_low[i] = (mix_rate * far_l[i].astype(jnp.float32)).T.astype(jnp.bfloat16)
        far_col[i] = jnp.broadcast_to(far_g[i], (128, early)).T
        for s in range(0, early, early // 2):
            r = pl.ds(s, early // 2)
            prod = jnp.dot(far_low[i, r, :], h_v[0], preferred_element_type=jnp.float32)
            new = (raw_v[i, r, :].astype(jnp.float32) + prod) * far_col[i, r, 0:1]
            o = pl.ds(pl.multiple_of(owner * rows + s, 8), early // 2)
            out_g[o, :] = (new * rf_v[0]).astype(jnp.bfloat16)

    for i, chunk in enumerate(raws):
        raw_move(0, chunk, 0, to_x).wait_recv()
        if i % 2 == 0:
            keep(raw_move(5, chunk, 0, to_y))
        raw_move(1, chunk, 0, to_y).wait_recv()
        if i % 2 == 1:
            keep(raw_move(5, chunk, 1, to_x))
    correct(0, to_x)
    correct(1, to_y)

    def relay(i, chunk, keep, forward):
        move(0, chunk, to_x, to_x).wait_recv()
        if i % 2 == 0:
            keep(move(5, chunk, to_x, to_y))
        if forward:
            keep(move(3, chunk, to_x, sib))
        move(1, chunk, to_y, to_y).wait_recv()
        if i % 2 == 1:
            keep(move(5, chunk, to_y, to_x))
        if forward:
            keep(move(4, chunk, to_y, sib))

    for i, chunk in enumerate(bulk):
        relay(i, chunk, keep, True)
        if i == 0:
            keep(move(3, block, to_x, sib))
            keep(move(4, block, to_y, sib))

    @pl.when(core == late)
    def _():
        for chunk in alone:
            move(0, chunk, me, to_x).start()
            move(1, chunk, me, to_y).start()

    for chunk in raws:
        raw_move(5, chunk, 0, to_x).wait_recv()
    small(far_l.at[0], far_l.at[2], 6, to_y).wait_recv()
    small(far_g.at[0], far_g.at[2], 9, to_y).wait_recv()
    correct(2, diag)
    for i, chunk in enumerate(bulk):
        move(5, chunk, diag, to_x).wait_recv()
        keep(move(6, chunk, diag, sib))
        if i == 0:
            keep(move(6, block, diag, sib))
    for chunk in [block] + bulk:
        move(2, chunk, sib, sib).wait_recv()
        move(3, chunk, to_x + flip, sib).wait_recv()
        move(4, chunk, to_y + flip, sib).wait_recv()
        move(6, chunk, diag + flip, sib).wait_recv()
    move(2, own_tail, sib, sib).wait_recv()

    @pl.when(core == late)
    def _():
        own = []

        def go(c):
            own.append(c)
            c.start()

        for i, chunk in enumerate(alone):
            relay(i, chunk, go, False)
        for chunk in alone:
            move(5, chunk, diag, to_x).wait_recv()
            move(0, chunk, me, to_x).wait_send()
            move(1, chunk, me, to_y).wait_send()
        for c in own:
            c.wait_send()

    for c in started:
        c.wait_send()


def tail_kernel(rows, unit, up, after, tail, ready, send, recv):
    solo = tail.shape[1]
    me, core, sib, to_x, to_y, diag, flip = place()
    chunks = pairs(0, unit, ALONE)
    whole = (0, solo)
    rest = (to_x, to_y, diag)
    barrier = pltpu.get_barrier_semaphore()

    def remote(src, dst, slot, i, target):
        return pltpu.make_async_remote_copy(
            src_ref=src, dst_ref=dst, send_sem=send.at[slot, i],
            recv_sem=recv.at[slot, i], device_id={AXIS: target})

    def held(owner, s, z):
        return up.at[pl.ds(pl.multiple_of(owner * rows + rows - solo + s, 8), z), :]

    def move(slot, i, chunk, owner, target, first=False):
        s, z = chunk
        dst = tail.at[owner, s:s + z, :]
        return remote(held(owner, s, z) if first else dst, dst, slot, i, target)

    def copy(owner):
        r = pl.ds(pl.multiple_of(owner * rows + rows - solo, 8), solo)
        tail[owner] = up[r, :]

    @pl.when(core != late)
    def _():
        started = []

        def keep(c):
            started.append(c)
            c.start()

        for d in (to_x, to_y, sib):
            pl.semaphore_signal(barrier, inc=1, device_id={AXIS: d})
        pl.semaphore_wait(barrier, 2)
        for i, c in enumerate(chunks):
            keep(move(0, i, c, me, to_x, True))
            keep(move(1, i, c, me, to_y, True))
        for i, c in enumerate(chunks):
            move(0, i, c, to_x, to_x).wait_recv()
            if i % 2 == 0:
                keep(move(5, i, c, to_x, to_y))
            move(1, i, c, to_y, to_y).wait_recv()
            if i % 2 == 1:
                keep(move(5, i, c, to_y, to_x))
        pl.semaphore_wait(ready, 1)
        keep(move(3, 0, whole, to_x, sib))
        keep(move(4, 0, whole, to_y, sib))
        for i, c in enumerate(chunks):
            move(5, i, c, diag, to_x).wait_recv()
            keep(move(6, i, c, diag, sib))
        for i, owner in enumerate(rest):
            move(7, i, whole, owner + flip, sib).wait_recv()
        for c in started:
            c.wait_send()

    @pl.when(core == late)
    def _():
        pl.semaphore_wait(barrier, 1)
        pl.semaphore_signal(ready, inc=1, device_id={AXIS: sib})
        out = [move(7, i, whole, owner, sib, True) for i, owner in enumerate(rest)]
        for c in out:
            c.start()
        for owner in rest:
            copy(owner)
        move(3, 0, whole, to_x + flip, sib).wait_recv()
        move(4, 0, whole, to_y + flip, sib).wait_recv()
        for i, c in enumerate(chunks):
            move(6, i, c, diag + flip, sib).wait_recv()
        for c in out:
            c.wait_send()


def write_kernel(rows, solo, a_v, b_v, fac, a_hbm, b_hbm, fa_hbm, fb_hbm, done, sem, fac_sem):
    done[...] = jnp.zeros_like(done)
    n = a_v.shape[0] // rows
    first = lax.axis_index(AXIS) // 2 * 2
    copies = [
        pltpu.make_async_copy(fac.at[i, 0], dst, fac_sem.at[i])
        for i, dst in enumerate((fa_hbm, fb_hbm))
    ]
    for k in range(n):
        for i, (src, dst) in enumerate(((a_v, a_hbm), (b_v, b_hbm))):
            owner = lax.rem(first + k, n)
            z = rows - solo if i and k > 1 else rows
            r = pl.ds(pl.multiple_of(owner * rows, 8), z)
            copies.append(pltpu.make_async_copy(src.at[r, :], dst.at[r, :], sem.at[i, k]))
    for c in copies:
        c.start()
    for c in copies:
        c.wait()


def finish_kernel(rows, tail, before, b_hbm, sem):
    n, solo, _ = tail.shape
    first = lax.axis_index(AXIS) // 2 * 2
    copies = []
    for k in range(2, n):
        owner = lax.rem(first + k, n)
        r = pl.ds(pl.multiple_of((owner + 1) * rows - solo, 8), solo)
        copies.append(pltpu.make_async_copy(tail.at[owner], b_hbm.at[r, :], sem.at[k]))
    for c in copies:
        c.start()
    for c in copies:
        c.wait()


def paired(n, weight_gate, low_gate, high_gate, weight_up, low_up, high_up, norm_gain):
    rows, cols = weight_gate.shape
    unit = rows // 40
    solo = 2 * sum(ALONE) * unit
    early = 2 * sum(RAW) * unit
    full = (n * rows, cols)
    vmem = pl.BlockSpec(memory_space=pltpu.VMEM)
    hbm = pl.BlockSpec(memory_space=pl.ANY)
    space = pl.BlockSpec(memory_space=pltpu.HBM)
    rank = high_gate.shape[0]
    grant = 65472 * 2**10 - (4 * full[0] * cols + 8 * cols) // 2**10 * 2**10 - 24 * 2**10
    slots = 20
    gate, up, fac = pl.pallas_call(
        functools.partial(gather_kernel, unit, solo),
        out_shape=(
            pltpu.VMEM(full, jnp.bfloat16),
            pltpu.VMEM(full, jnp.bfloat16),
            pltpu.VMEM((2, 1, cols), jnp.float32),
        ),
        in_specs=[space] * 7,
        out_specs=(vmem, vmem, vmem),
        scratch_shapes=[
            pltpu.VMEM((2, rows, cols), jnp.bfloat16),
            pltpu.VMEM((2, rank, rows), jnp.bfloat16),
            pltpu.VMEM((2, rank, cols), jnp.bfloat16),
            pltpu.VMEM((1, rows), jnp.float32),
            pltpu.VMEM((2, rows, rank), jnp.bfloat16),
            pltpu.VMEM((2, rows, cols), jnp.float32),
            pltpu.VMEM((rows, 128), jnp.float32),
            pltpu.VMEM((2, 1, cols), jnp.float32),
            pltpu.VMEM((4, 1, cols), jnp.float32),
            pltpu.VMEM((3, 1, cols), jnp.float32),
            pltpu.VMEM((2, 1, cols), jnp.float32),
            pltpu.VMEM((3, early, cols), jnp.bfloat16),
            pltpu.VMEM((3, rank, early), jnp.bfloat16),
            pltpu.VMEM((3, 1, early), jnp.float32),
            pltpu.VMEM((3, early, rank), jnp.bfloat16),
            pltpu.VMEM((3, early, 128), jnp.float32),
            pltpu.SemaphoreType.DMA((7,)),
            pltpu.SemaphoreType.DMA((10,)),
            pltpu.SemaphoreType.DMA((10,)),
            pltpu.SemaphoreType.DMA((7, slots)),
            pltpu.SemaphoreType.DMA((7, slots)),
        ],
        compiler_params=pltpu.CompilerParams(
            collective_id=0, has_side_effects=True, vmem_limit_bytes=grant
        ),
        name="merge_gather",
    )(weight_gate, weight_up, low_gate.T, low_up.T, high_gate, high_up, norm_gain)
    whole = jax.ShapeDtypeStruct(full, jnp.bfloat16)
    ready_gate, ready_up, factor_gate, factor_up, done = pl.pallas_call(
        functools.partial(write_kernel, rows, solo),
        out_shape=(whole, whole) + (jax.ShapeDtypeStruct((cols,), jnp.float32),) * 2
        + (pltpu.VMEM((8, 128), jnp.float32),),
        in_specs=[vmem, vmem, vmem],
        out_specs=(hbm,) * 4 + (vmem,),
        scratch_shapes=[pltpu.SemaphoreType.DMA((2, n)), pltpu.SemaphoreType.DMA((2,))],
        compiler_params=pltpu.CompilerParams(vmem_limit_bytes=2**20),
        name="write_out",
    )(gate, up, fac)
    tail = pl.pallas_call(
        functools.partial(tail_kernel, rows, unit),
        out_shape=pltpu.VMEM((n, solo, cols), jnp.bfloat16),
        in_specs=[vmem, vmem],
        out_specs=vmem,
        scratch_shapes=[
            pltpu.SemaphoreType.REGULAR,
            pltpu.SemaphoreType.DMA((8, 2 * len(ALONE))),
            pltpu.SemaphoreType.DMA((8, 2 * len(ALONE))),
        ],
        compiler_params=pltpu.CompilerParams(
            collective_id=1, has_side_effects=True, vmem_limit_bytes=2**20
        ),
        name="tail_gather",
    )(up, done)
    ready_up = pl.pallas_call(
        functools.partial(finish_kernel, rows),
        out_shape=whole,
        in_specs=[vmem, hbm],
        out_specs=hbm,
        input_output_aliases={1: 0},
        scratch_shapes=[pltpu.SemaphoreType.DMA((n,))],
        compiler_params=pltpu.CompilerParams(vmem_limit_bytes=2**20),
        name="finish",
    )(tail, ready_up)
    return ready_gate, ready_up, factor_gate, factor_up


def solution(mesh):
    in_specs = (
        P("shard", "tp"),
        P("shard", None),
        P(None, "tp"),
        P("shard", "tp"),
        P("shard", None),
        P(None, "tp"),
        P("shard"),
    )
    out_specs = (P(None, "tp"), P(None, "tp"), P("tp"), P("tp"))
    n = mesh.shape[AXIS]
    side = math.isqrt(n // 2)
    body = functools.partial(paired, n) if side == 2 and 2 * side * side == n else local
    return jax.shard_map(body, mesh=mesh, in_specs=in_specs, out_specs=out_specs, check_vma=False)
```

```python
import functools
import math

import jax
import jax.numpy as jnp
from jax import lax
from jax.experimental import pallas as pl
from jax.experimental.pallas import tpu as pltpu
from jax.sharding import PartitionSpec as P

mix_rate = 2.0
AXIS = "shard"


def local(weight_gate, low_gate, high_gate, weight_up, low_up, high_up, norm_gain):
    latest_gate = weight_gate.astype(jnp.float32) + mix_rate * jnp.dot(
        low_gate, high_gate, preferred_element_type=jnp.float32
    )
    latest_up = weight_up.astype(jnp.float32) + mix_rate * jnp.dot(
        low_up, high_up, preferred_element_type=jnp.float32
    )
    latest_gained_gate = latest_gate * norm_gain[:, None]
    latest_gained_up = latest_up * norm_gain[:, None]
    total_gate, total_up = lax.psum(
        (
            jnp.sum(latest_gained_gate * latest_gained_gate, axis=0),
            jnp.sum(latest_gained_up * latest_gained_up, axis=0),
        ),
        AXIS,
    )
    factor_gate = jnp.sqrt(total_gate)
    factor_up = jnp.sqrt(total_up)
    narrow_gate = (latest_gained_gate / factor_gate).astype(jnp.bfloat16)
    narrow_up = (latest_gained_up / factor_up).astype(jnp.bfloat16)
    ready_gate = lax.all_gather(narrow_gate, AXIS, axis=0, tiled=True)
    ready_up = lax.all_gather(narrow_up, AXIS, axis=0, tiled=True)
    return (ready_gate, ready_up, factor_gate, factor_up)


late = 0
RAW = (4, 4)
GATE = (12,)
UP = (4, 4)
ALONE = (8, 4)


def place():
    me = lax.axis_index(AXIS)
    core = lax.rem(me, 2)
    x = lax.rem(me // 2, 2)
    y = me // 4
    to_x = me + 2 - 4 * x
    to_y = me + 4 - 8 * y
    return me, core, me + 1 - 2 * core, to_x, to_y, to_x + 4 - 8 * y, 1 - 2 * core


def pairs(start, unit, sizes):
    out = []
    for z in sizes:
        for _ in range(2):
            out.append((start, z * unit))
            start += z * unit
    return out


def gather_kernel(
    unit, solo, wg_hbm, wu_hbm, lg_hbm, lu_hbm, hg_hbm, hu_hbm, gain_hbm,
    out_g, out_u, fac,
    w_v, l_v, h_v, gain_v, low_v, g_v, col_v, part, mine, heard, rf_v,
    raw_v, far_l, far_g, far_low, far_col,
    in_sem, small_send, small_recv, send, recv,
):
    rows, cols = wg_hbm.shape
    me, core, sib, to_x, to_y, diag, flip = place()
    early = 2 * sum(RAW) * unit
    shared_up = rows - solo
    raws = [(0, s, z) for s, z in pairs(0, unit, RAW)]
    bulk = [(0, s, z) for s, z in pairs(early, unit, GATE)]
    bulk += [(1, s, z) for s, z in pairs(0, unit, UP)]
    alone = [(1, s, z) for s, z in pairs(shared_up, unit, ALONE)]
    own_tail = (1, shared_up, solo)
    block = (0, 0, early)
    every = raws + bulk
    order = {c: i for i, c in enumerate(every + alone + [block, own_tail])}
    outs = (out_g, out_u)

    barrier = pltpu.get_barrier_semaphore()
    for d in (to_x, to_y, sib):
        pl.semaphore_signal(barrier, inc=1, device_id={AXIS: d})

    gain_load = pltpu.make_async_copy(gain_hbm, gain_v.at[0], in_sem.at[6])
    low_loads, high_loads = (
        [
            pltpu.make_async_copy(src, dst.at[a], in_sem.at[3 * a + i])
            for a, src in enumerate(pair)
        ]
        for i, (pair, dst) in enumerate((((lg_hbm, lu_hbm), l_v), ((hg_hbm, hu_hbm), h_v)))
    )
    loads = [
        pltpu.make_async_copy(wg_hbm.at[early:, :], w_v.at[0, early:, :], in_sem.at[2]),
        pltpu.make_async_copy(wu_hbm, w_v.at[1], in_sem.at[5]),
    ]
    raw_loads = [
        pltpu.make_async_copy(wg_hbm.at[s:s + z, :], w_v.at[0, s:s + z, :], in_sem.at[7 + i])
        for i, (_, s, z) in enumerate(raws)
    ]
    for c in raw_loads[:2] + [low_loads[0], gain_load, high_loads[0]] + raw_loads[2:]:
        c.start()
    for c in (loads[0], low_loads[1], high_loads[1], loads[1]):
        c.start()

    started = []

    def keep(c):
        started.append(c)
        c.start()

    def remote(src, dst, slot, chunk, target):
        i = order[chunk]
        return pltpu.make_async_remote_copy(
            src_ref=src, dst_ref=dst, send_sem=send.at[slot, i],
            recv_sem=recv.at[slot, i], device_id={AXIS: target})

    def small(src, dst, i, target):
        return pltpu.make_async_remote_copy(
            src_ref=src, dst_ref=dst, send_sem=small_send.at[i],
            recv_sem=small_recv.at[i], device_id={AXIS: target})

    def piece(chunk, owner):
        a, s, z = chunk
        return outs[a].at[pl.ds(pl.multiple_of(owner * rows + s, 8), z), :]

    def move(slot, chunk, owner, target):
        p = piece(chunk, owner)
        return remote(p, p, slot, chunk, target)

    def raw_move(slot, chunk, at, target):
        _, s, z = chunk
        src = w_v.at[0, s:s + z, :] if slot < 2 else raw_v.at[at, s:s + z, :]
        return remote(src, raw_v.at[slot if slot < 2 else 2, s:s + z, :], slot, chunk, target)

    pl.semaphore_wait(barrier, 3)
    for c, chunk in list(zip(raw_loads, raws))[:2]:
        c.wait()
        keep(raw_move(0, chunk, 0, to_x))
        keep(raw_move(1, chunk, 0, to_y))
    low_own, gain_own = l_v.at[0, :, :early], gain_v.at[:, :early]
    low_loads[0].wait()
    gain_load.wait()
    for i, d in enumerate((to_x, to_y)):
        keep(small(low_own, far_l.at[i], 4 + i, d))
        keep(small(gain_own, far_g.at[i], 7 + i, d))

    col_v[...] = jnp.broadcast_to(gain_v[...], (128, rows)).T
    step = rows // 5
    for a in range(2):
        if a:
            low_loads[a].wait()
        else:
            for c in raw_loads[2:]:
                c.wait()
        low_v[a] = (mix_rate * l_v[a].astype(jnp.float32)).T.astype(jnp.bfloat16)
        high_loads[a].wait()
        loads[a].wait()
        acc = jnp.zeros((8, cols), jnp.float32)
        for s in range(0, rows, step):
            r = pl.ds(s, step)
            prod = jnp.dot(low_v[a, r, :], h_v[a], preferred_element_type=jnp.float32)
            new = (w_v[a, r, :].astype(jnp.float32) + prod) * col_v[r, 0:1]
            g_v[a, r, :] = new
            acc = acc + jnp.sum((new * new).reshape(step // 8, 8, cols), axis=0)
        part[a] = jnp.sum(acc, axis=0, keepdims=True)

    sum_pair = small(part, heard.at[0], 0, sib)
    sum_x = small(mine.at[0], heard.at[1], 1, to_x)
    sum_y = small(mine.at[1], heard.at[2], 2, to_y)
    sum_all = small(mine.at[2], mine.at[2], 3, sib)

    @pl.when(core == late)
    def _():
        sum_pair.start()
        for chunk in raws[2:]:
            raw_move(0, chunk, 0, to_x).start()
            raw_move(1, chunk, 0, to_y).start()
        sum_all.wait_recv()

    @pl.when(core != late)
    def _():
        sum_pair.wait_recv()
        mine[0] = part[...] + heard[0]
        raw_move(1, raws[2], 0, to_y).start()
        sum_x.start()
        raw_move(0, raws[2], 0, to_x).start()
        sum_x.wait_recv()
        mine[1] = mine[0] + heard[1]
        raw_move(0, raws[3], 0, to_x).start()
        sum_y.start()
        raw_move(1, raws[3], 0, to_y).start()
        sum_y.wait_recv()
        mine[2] = mine[1] + heard[2]
        sum_all.start()

    for chunk in raws[2:]:
        started.append(raw_move(0, chunk, 0, to_x))
        started.append(raw_move(1, chunk, 0, to_y))
    for a in range(2):
        factor = jnp.sqrt(mine[2, a])
        fac[a] = factor
        rf_v[a] = 1.0 / factor

    def scale(chunk):
        a, s, z = chunk
        r = pl.ds(pl.multiple_of(me * rows + s, 8), z)
        outs[a][r, :] = (g_v[a, s:s + z, :] * rf_v[a]).astype(jnp.bfloat16)

    def send_own(chunk):
        keep(move(0, chunk, me, to_x))
        keep(move(1, chunk, me, to_y))
        keep(move(2, chunk, me, sib))

    for i, chunk in enumerate(bulk):
        scale(chunk)
        if i:
            send_own(bulk[i - 1])
    scale(block)
    send_own(bulk[-1])
    for chunk in alone:
        scale(chunk)
    keep(move(2, block, me, sib))
    keep(move(2, own_tail, me, sib))

    low_x, low_y = (small(low_own, far_l.at[i], 4 + i, to_x) for i in range(2))
    gain_x, gain_y = (small(gain_own, far_g.at[i], 7 + i, to_x) for i in range(2))
    low_x.wait_recv()
    keep(small(far_l.at[0], far_l.at[2], 6, to_y))
    gain_x.wait_recv()
    keep(small(far_g.at[0], far_g.at[2], 9, to_y))
    low_y.wait_recv()
    gain_y.wait_recv()

    def correct(i, owner):
        far_low[i] = (mix_rate * far_l[i].astype(jnp.float32)).T.astype(jnp.bfloat16)
        far_col[i] = jnp.broadcast_to(far_g[i], (128, early)).T
        for s in range(0, early, early // 2):
            r = pl.ds(s, early // 2)
            prod = jnp.dot(far_low[i, r, :], h_v[0], preferred_element_type=jnp.float32)
            new = (raw_v[i, r, :].astype(jnp.float32) + prod) * far_col[i, r, 0:1]
            o = pl.ds(pl.multiple_of(owner * rows + s, 8), early // 2)
            out_g[o, :] = (new * rf_v[0]).astype(jnp.bfloat16)

    for i, chunk in enumerate(raws):
        raw_move(0, chunk, 0, to_x).wait_recv()
        if i % 2 == 0:
            keep(raw_move(5, chunk, 0, to_y))
        raw_move(1, chunk, 0, to_y).wait_recv()
        if i % 2 == 1:
            keep(raw_move(5, chunk, 1, to_x))
    correct(0, to_x)
    correct(1, to_y)

    def relay(i, chunk, keep, forward):
        move(0, chunk, to_x, to_x).wait_recv()
        if i % 2 == 0:
            keep(move(5, chunk, to_x, to_y))
        if forward:
            keep(move(3, chunk, to_x, sib))
        move(1, chunk, to_y, to_y).wait_recv()
        if i % 2 == 1:
            keep(move(5, chunk, to_y, to_x))
        if forward:
            keep(move(4, chunk, to_y, sib))

    for i, chunk in enumerate(bulk):
        relay(i, chunk, keep, True)
        if i == 0:
            keep(move(3, block, to_x, sib))
            keep(move(4, block, to_y, sib))

    @pl.when(core == late)
    def _():
        for chunk in alone:
            move(0, chunk, me, to_x).start()
            move(1, chunk, me, to_y).start()

    for chunk in raws:
        raw_move(5, chunk, 0, to_x).wait_recv()
    small(far_l.at[0], far_l.at[2], 6, to_y).wait_recv()
    small(far_g.at[0], far_g.at[2], 9, to_y).wait_recv()
    correct(2, diag)
    for i, chunk in enumerate(bulk):
        move(5, chunk, diag, to_x).wait_recv()
        keep(move(6, chunk, diag, sib))
        if i == 0:
            keep(move(6, block, diag, sib))
    for chunk in [block] + bulk:
        move(2, chunk, sib, sib).wait_recv()
        move(3, chunk, to_x + flip, sib).wait_recv()
        move(4, chunk, to_y + flip, sib).wait_recv()
        move(6, chunk, diag + flip, sib).wait_recv()
    move(2, own_tail, sib, sib).wait_recv()

    @pl.when(core == late)
    def _():
        own = []

        def go(c):
            own.append(c)
            c.start()

        for i, chunk in enumerate(alone):
            relay(i, chunk, go, False)
        for chunk in alone:
            move(5, chunk, diag, to_x).wait_recv()
            move(0, chunk, me, to_x).wait_send()
            move(1, chunk, me, to_y).wait_send()
        for c in own + [sum_pair]:
            c.wait_send()

    @pl.when(core != late)
    def _():
        for c in (sum_x, sum_y, sum_all):
            c.wait_send()

    for c in started:
        c.wait_send()


def tail_kernel(rows, unit, up, after, tail, ready, send, recv):
    solo = tail.shape[1]
    me, core, sib, to_x, to_y, diag, flip = place()
    chunks = pairs(0, unit, ALONE)
    whole = (0, solo)
    rest = (to_x, to_y, diag)
    barrier = pltpu.get_barrier_semaphore()

    def remote(src, dst, slot, i, target):
        return pltpu.make_async_remote_copy(
            src_ref=src, dst_ref=dst, send_sem=send.at[slot, i],
            recv_sem=recv.at[slot, i], device_id={AXIS: target})

    def held(owner, s, z):
        return up.at[pl.ds(pl.multiple_of(owner * rows + rows - solo + s, 8), z), :]

    def move(slot, i, chunk, owner, target, first=False):
        s, z = chunk
        dst = tail.at[owner, s:s + z, :]
        return remote(held(owner, s, z) if first else dst, dst, slot, i, target)

    def copy(owner):
        r = pl.ds(pl.multiple_of(owner * rows + rows - solo, 8), solo)
        tail[owner] = up[r, :]

    @pl.when(core != late)
    def _():
        started = []

        def keep(c):
            started.append(c)
            c.start()

        for d in (to_x, to_y, sib):
            pl.semaphore_signal(barrier, inc=1, device_id={AXIS: d})
        pl.semaphore_wait(barrier, 2)
        for i, c in enumerate(chunks):
            keep(move(0, i, c, me, to_x, True))
            keep(move(1, i, c, me, to_y, True))
        for i, c in enumerate(chunks):
            move(0, i, c, to_x, to_x).wait_recv()
            if i % 2 == 0:
                keep(move(5, i, c, to_x, to_y))
            move(1, i, c, to_y, to_y).wait_recv()
            if i % 2 == 1:
                keep(move(5, i, c, to_y, to_x))
        pl.semaphore_wait(ready, 1)
        keep(move(3, 0, whole, to_x, sib))
        keep(move(4, 0, whole, to_y, sib))
        for i, c in enumerate(chunks):
            move(5, i, c, diag, to_x).wait_recv()
            keep(move(6, i, c, diag, sib))
        for i, owner in enumerate(rest):
            move(7, i, whole, owner + flip, sib).wait_recv()
        for c in started:
            c.wait_send()

    @pl.when(core == late)
    def _():
        pl.semaphore_wait(barrier, 1)
        pl.semaphore_signal(ready, inc=1, device_id={AXIS: sib})
        out = [move(7, i, whole, owner, sib, True) for i, owner in enumerate(rest)]
        for c in out:
            c.start()
        for owner in rest:
            copy(owner)
        move(3, 0, whole, to_x + flip, sib).wait_recv()
        move(4, 0, whole, to_y + flip, sib).wait_recv()
        for i, c in enumerate(chunks):
            move(6, i, c, diag + flip, sib).wait_recv()
        for c in out:
            c.wait_send()


def write_kernel(rows, solo, a_v, b_v, fac, a_hbm, b_hbm, fa_hbm, fb_hbm, done, sem, fac_sem):
    done[...] = jnp.zeros_like(done)
    n = a_v.shape[0] // rows
    first = lax.axis_index(AXIS) // 2 * 2
    copies = [
        pltpu.make_async_copy(fac.at[i, 0], dst, fac_sem.at[i])
        for i, dst in enumerate((fa_hbm, fb_hbm))
    ]
    for k in range(n):
        for i, (src, dst) in enumerate(((a_v, a_hbm), (b_v, b_hbm))):
            owner = lax.rem(first + k, n)
            z = rows - solo if i and k > 1 else rows
            r = pl.ds(pl.multiple_of(owner * rows, 8), z)
            copies.append(pltpu.make_async_copy(src.at[r, :], dst.at[r, :], sem.at[i, k]))
    for c in copies:
        c.start()
    for c in copies:
        c.wait()


def finish_kernel(rows, tail, before, b_hbm, sem):
    n, solo, _ = tail.shape
    first = lax.axis_index(AXIS) // 2 * 2
    copies = []
    for k in range(2, n):
        owner = lax.rem(first + k, n)
        r = pl.ds(pl.multiple_of((owner + 1) * rows - solo, 8), solo)
        copies.append(pltpu.make_async_copy(tail.at[owner], b_hbm.at[r, :], sem.at[k]))
    for c in copies:
        c.start()
    for c in copies:
        c.wait()


def paired(n, weight_gate, low_gate, high_gate, weight_up, low_up, high_up, norm_gain):
    rows, cols = weight_gate.shape
    unit = rows // 40
    solo = 2 * sum(ALONE) * unit
    early = 2 * sum(RAW) * unit
    full = (n * rows, cols)
    vmem = pl.BlockSpec(memory_space=pltpu.VMEM)
    hbm = pl.BlockSpec(memory_space=pl.ANY)
    space = pl.BlockSpec(memory_space=pltpu.HBM)
    rank = high_gate.shape[0]
    grant = 65472 * 2**10 - (4 * full[0] * cols + 8 * cols) // 2**10 * 2**10 - 24 * 2**10
    slots = 20
    gate, up, fac = pl.pallas_call(
        functools.partial(gather_kernel, unit, solo),
        out_shape=(
            pltpu.VMEM(full, jnp.bfloat16),
            pltpu.VMEM(full, jnp.bfloat16),
            pltpu.VMEM((2, 1, cols), jnp.float32),
        ),
        in_specs=[space] * 7,
        out_specs=(vmem, vmem, vmem),
        scratch_shapes=[
            pltpu.VMEM((2, rows, cols), jnp.bfloat16),
            pltpu.VMEM((2, rank, rows), jnp.bfloat16),
            pltpu.VMEM((2, rank, cols), jnp.bfloat16),
            pltpu.VMEM((1, rows), jnp.float32),
            pltpu.VMEM((2, rows, rank), jnp.bfloat16),
            pltpu.VMEM((2, rows, cols), jnp.float32),
            pltpu.VMEM((rows, 128), jnp.float32),
            pltpu.VMEM((2, 1, cols), jnp.float32),
            pltpu.VMEM((3, 2, 1, cols), jnp.float32),
            pltpu.VMEM((3, 2, 1, cols), jnp.float32),
            pltpu.VMEM((2, 1, cols), jnp.float32),
            pltpu.VMEM((3, early, cols), jnp.bfloat16),
            pltpu.VMEM((3, rank, early), jnp.bfloat16),
            pltpu.VMEM((3, 1, early), jnp.float32),
            pltpu.VMEM((3, early, rank), jnp.bfloat16),
            pltpu.VMEM((3, early, 128), jnp.float32),
            pltpu.SemaphoreType.DMA((7 + 2 * len(RAW),)),
            pltpu.SemaphoreType.DMA((10,)),
            pltpu.SemaphoreType.DMA((10,)),
            pltpu.SemaphoreType.DMA((7, slots)),
            pltpu.SemaphoreType.DMA((7, slots)),
        ],
        compiler_params=pltpu.CompilerParams(
            collective_id=0, has_side_effects=True, vmem_limit_bytes=grant
        ),
        name="merge_gather",
    )(weight_gate, weight_up, low_gate.T, low_up.T, high_gate, high_up, norm_gain)
    whole = jax.ShapeDtypeStruct(full, jnp.bfloat16)
    ready_gate, ready_up, factor_gate, factor_up, done = pl.pallas_call(
        functools.partial(write_kernel, rows, solo),
        out_shape=(whole, whole) + (jax.ShapeDtypeStruct((cols,), jnp.float32),) * 2
        + (pltpu.VMEM((8, 128), jnp.float32),),
        in_specs=[vmem, vmem, vmem],
        out_specs=(hbm,) * 4 + (vmem,),
        scratch_shapes=[pltpu.SemaphoreType.DMA((2, n)), pltpu.SemaphoreType.DMA((2,))],
        compiler_params=pltpu.CompilerParams(vmem_limit_bytes=2**20),
        name="write_out",
    )(gate, up, fac)
    tail = pl.pallas_call(
        functools.partial(tail_kernel, rows, unit),
        out_shape=pltpu.VMEM((n, solo, cols), jnp.bfloat16),
        in_specs=[vmem, vmem],
        out_specs=vmem,
        scratch_shapes=[
            pltpu.SemaphoreType.REGULAR,
            pltpu.SemaphoreType.DMA((8, 2 * len(ALONE))),
            pltpu.SemaphoreType.DMA((8, 2 * len(ALONE))),
        ],
        compiler_params=pltpu.CompilerParams(
            collective_id=1, has_side_effects=True, vmem_limit_bytes=2**20
        ),
        name="tail_gather",
    )(up, done)
    ready_up = pl.pallas_call(
        functools.partial(finish_kernel, rows),
        out_shape=whole,
        in_specs=[vmem, hbm],
        out_specs=hbm,
        input_output_aliases={1: 0},
        scratch_shapes=[pltpu.SemaphoreType.DMA((n,))],
        compiler_params=pltpu.CompilerParams(vmem_limit_bytes=2**20),
        name="finish",
    )(tail, ready_up)
    return ready_gate, ready_up, factor_gate, factor_up


def solution(mesh):
    in_specs = (
        P("shard", "tp"),
        P("shard", None),
        P(None, "tp"),
        P("shard", "tp"),
        P("shard", None),
        P(None, "tp"),
        P("shard"),
    )
    out_specs = (P(None, "tp"), P(None, "tp"), P("tp"), P("tp"))
    n = mesh.shape[AXIS]
    side = math.isqrt(n // 2)
    body = functools.partial(paired, n) if side == 2 and 2 * side * side == n else local
    return jax.shard_map(body, mesh=mesh, in_specs=in_specs, out_specs=out_specs, check_vma=False)
```

```python
import functools
import math

import jax
import jax.numpy as jnp
from jax import lax
from jax.experimental import pallas as pl
from jax.experimental.pallas import tpu as pltpu
from jax.sharding import PartitionSpec as P

mix_rate = 2.0
AXIS = "shard"


def local(weight_gate, low_gate, high_gate, weight_up, low_up, high_up, norm_gain):
    latest_gate = weight_gate.astype(jnp.float32) + mix_rate * jnp.dot(
        low_gate, high_gate, preferred_element_type=jnp.float32
    )
    latest_up = weight_up.astype(jnp.float32) + mix_rate * jnp.dot(
        low_up, high_up, preferred_element_type=jnp.float32
    )
    latest_gained_gate = latest_gate * norm_gain[:, None]
    latest_gained_up = latest_up * norm_gain[:, None]
    total_gate, total_up = lax.psum(
        (
            jnp.sum(latest_gained_gate * latest_gained_gate, axis=0),
            jnp.sum(latest_gained_up * latest_gained_up, axis=0),
        ),
        AXIS,
    )
    factor_gate = jnp.sqrt(total_gate)
    factor_up = jnp.sqrt(total_up)
    narrow_gate = (latest_gained_gate / factor_gate).astype(jnp.bfloat16)
    narrow_up = (latest_gained_up / factor_up).astype(jnp.bfloat16)
    ready_gate = lax.all_gather(narrow_gate, AXIS, axis=0, tiled=True)
    ready_up = lax.all_gather(narrow_up, AXIS, axis=0, tiled=True)
    return (ready_gate, ready_up, factor_gate, factor_up)


late = 0
RAW = (4, 4)
GATE = (12,)
UP = (4, 4)
ALONE = (8, 4)


def place():
    me = lax.axis_index(AXIS)
    core = lax.rem(me, 2)
    x = lax.rem(me // 2, 2)
    y = me // 4
    to_x = me + 2 - 4 * x
    to_y = me + 4 - 8 * y
    return me, core, me + 1 - 2 * core, to_x, to_y, to_x + 4 - 8 * y, 1 - 2 * core


def pairs(start, unit, sizes):
    out = []
    for z in sizes:
        for _ in range(2):
            out.append((start, z * unit))
            start += z * unit
    return out


def gather_kernel(
    unit, solo, wg_hbm, wu_hbm, lg_hbm, lu_hbm, hg_hbm, hu_hbm, gain_hbm,
    out_g, out_u, fac,
    w_v, l_v, h_v, gain_v, low_v, g_v, col_v, part, mine, heard, rf_v,
    raw_v, far_l, far_g, far_low, far_col,
    in_sem, small_send, small_recv, sent, crossed, recv,
):
    rows, cols = wg_hbm.shape
    me, core, sib, to_x, to_y, diag, flip = place()
    early = 2 * sum(RAW) * unit
    shared_up = rows - solo
    raws = [(0, s, z) for s, z in pairs(0, unit, RAW)]
    bulk = [(0, s, z) for s, z in pairs(early, unit, GATE)]
    bulk += [(1, s, z) for s, z in pairs(0, unit, UP)]
    alone = [(1, s, z) for s, z in pairs(shared_up, unit, ALONE)]
    own_tail = (1, shared_up, solo)
    block = (0, 0, early)
    every = raws + bulk
    order = {c: i for i, c in enumerate(every + alone)}
    lanes = {0: 0, 1: 1, 5: 2}
    outs = (out_g, out_u)

    barrier = pltpu.get_barrier_semaphore()
    for d in (to_x, to_y, sib):
        pl.semaphore_signal(barrier, inc=1, device_id={AXIS: d})

    gain_load = pltpu.make_async_copy(gain_hbm, gain_v.at[0], in_sem.at[6])
    low_loads, high_loads = (
        [
            pltpu.make_async_copy(src, dst.at[a], in_sem.at[3 * a + i])
            for a, src in enumerate(pair)
        ]
        for i, (pair, dst) in enumerate((((lg_hbm, lu_hbm), l_v), ((hg_hbm, hu_hbm), h_v)))
    )
    loads = [
        pltpu.make_async_copy(wg_hbm.at[early:, :], w_v.at[0, early:, :], in_sem.at[2]),
        pltpu.make_async_copy(wu_hbm, w_v.at[1], in_sem.at[5]),
    ]
    raw_loads = [
        pltpu.make_async_copy(wg_hbm.at[s:s + z, :], w_v.at[0, s:s + z, :], in_sem.at[7 + i])
        for i, (_, s, z) in enumerate(raws)
    ]
    for c in raw_loads[:2] + [low_loads[0], gain_load, high_loads[0]] + raw_loads[2:]:
        c.start()
    for c in (loads[0], low_loads[1], high_loads[1], loads[1]):
        c.start()

    started = []

    def keep(c):
        started.append(c)
        c.start()

    def go(c):
        c.start()

    def remote(src, dst, slot, chunk, target):
        if slot in lanes:
            got = recv.at[lanes[slot], order[chunk]]
            out = sent.at[1 if chunk in alone else 0]
        else:
            got, out = crossed, sent.at[2]
        return pltpu.make_async_remote_copy(
            src_ref=src, dst_ref=dst, send_sem=out, recv_sem=got, device_id={AXIS: target})

    def all_of(count, out):
        part = out_g.at[0:count, :]
        return pltpu.make_async_remote_copy(
            src_ref=part, dst_ref=part, send_sem=sent.at[out], recv_sem=crossed,
            device_id={AXIS: sib})

    def small(src, dst, i, target):
        return pltpu.make_async_remote_copy(
            src_ref=src, dst_ref=dst, send_sem=small_send.at[i],
            recv_sem=small_recv.at[i], device_id={AXIS: target})

    def piece(chunk, owner):
        a, s, z = chunk
        return outs[a].at[pl.ds(pl.multiple_of(owner * rows + s, 8), z), :]

    def move(slot, chunk, owner, target):
        p = piece(chunk, owner)
        return remote(p, p, slot, chunk, target)

    def raw_move(slot, chunk, at, target):
        _, s, z = chunk
        src = w_v.at[0, s:s + z, :] if slot < 2 else raw_v.at[at, s:s + z, :]
        return remote(src, raw_v.at[slot if slot < 2 else 2, s:s + z, :], slot, chunk, target)

    pl.semaphore_wait(barrier, 3)
    for c, chunk in list(zip(raw_loads, raws))[:2]:
        c.wait()
        go(raw_move(0, chunk, 0, to_x))
        go(raw_move(1, chunk, 0, to_y))
    low_own, gain_own = l_v.at[0, :, :early], gain_v.at[:, :early]
    low_loads[0].wait()
    gain_load.wait()
    for i, d in enumerate((to_x, to_y)):
        keep(small(low_own, far_l.at[i], 4 + i, d))
        keep(small(gain_own, far_g.at[i], 7 + i, d))

    col_v[...] = jnp.broadcast_to(gain_v[...], (128, rows)).T
    step = rows // 5
    for a in range(2):
        if a:
            low_loads[a].wait()
        else:
            for c in raw_loads[2:]:
                c.wait()
        low_v[a] = (mix_rate * l_v[a].astype(jnp.float32)).T.astype(jnp.bfloat16)
        high_loads[a].wait()
        loads[a].wait()
        acc = jnp.zeros((8, cols), jnp.float32)
        for s in range(0, rows, step):
            r = pl.ds(s, step)
            prod = jnp.dot(low_v[a, r, :], h_v[a], preferred_element_type=jnp.float32)
            new = (w_v[a, r, :].astype(jnp.float32) + prod) * col_v[r, 0:1]
            g_v[a, r, :] = new
            acc = acc + jnp.sum((new * new).reshape(step // 8, 8, cols), axis=0)
        part[a] = jnp.sum(acc, axis=0, keepdims=True)

    sum_pair = small(part, heard.at[0], 0, sib)
    sum_x = small(mine.at[0], heard.at[1], 1, to_x)
    sum_y = small(mine.at[1], heard.at[2], 2, to_y)
    sum_all = small(mine.at[2], mine.at[2], 3, sib)

    @pl.when(core == late)
    def _():
        sum_pair.start()
        for chunk in raws[2:]:
            raw_move(0, chunk, 0, to_x).start()
            raw_move(1, chunk, 0, to_y).start()
        sum_all.wait_recv()

    @pl.when(core != late)
    def _():
        sum_pair.wait_recv()
        mine[0] = part[...] + heard[0]
        raw_move(1, raws[2], 0, to_y).start()
        sum_x.start()
        raw_move(0, raws[2], 0, to_x).start()
        sum_x.wait_recv()
        mine[1] = mine[0] + heard[1]
        raw_move(0, raws[3], 0, to_x).start()
        sum_y.start()
        raw_move(1, raws[3], 0, to_y).start()
        sum_y.wait_recv()
        mine[2] = mine[1] + heard[2]
        sum_all.start()

    for a in range(2):
        factor = jnp.sqrt(mine[2, a])
        fac[a] = factor
        rf_v[a] = 1.0 / factor

    def scale(chunk):
        a, s, z = chunk
        r = pl.ds(pl.multiple_of(me * rows + s, 8), z)
        outs[a][r, :] = (g_v[a, s:s + z, :] * rf_v[a]).astype(jnp.bfloat16)

    def send_own(chunk):
        go(move(0, chunk, me, to_x))
        go(move(1, chunk, me, to_y))
        go(move(2, chunk, me, sib))

    for i, chunk in enumerate(bulk):
        scale(chunk)
        if i:
            send_own(bulk[i - 1])
    scale(block)
    send_own(bulk[-1])
    for chunk in alone:
        scale(chunk)
    go(move(2, block, me, sib))
    go(move(2, own_tail, me, sib))

    low_x, low_y = (small(low_own, far_l.at[i], 4 + i, to_x) for i in range(2))
    gain_x, gain_y = (small(gain_own, far_g.at[i], 7 + i, to_x) for i in range(2))
    low_x.wait_recv()
    keep(small(far_l.at[0], far_l.at[2], 6, to_y))
    gain_x.wait_recv()
    keep(small(far_g.at[0], far_g.at[2], 9, to_y))
    low_y.wait_recv()
    gain_y.wait_recv()

    def correct(i, owner):
        far_low[i] = (mix_rate * far_l[i].astype(jnp.float32)).T.astype(jnp.bfloat16)
        far_col[i] = jnp.broadcast_to(far_g[i], (128, early)).T
        for s in range(0, early, early // 2):
            r = pl.ds(s, early // 2)
            prod = jnp.dot(far_low[i, r, :], h_v[0], preferred_element_type=jnp.float32)
            new = (raw_v[i, r, :].astype(jnp.float32) + prod) * far_col[i, r, 0:1]
            o = pl.ds(pl.multiple_of(owner * rows + s, 8), early // 2)
            out_g[o, :] = (new * rf_v[0]).astype(jnp.bfloat16)

    for i, chunk in enumerate(raws):
        raw_move(0, chunk, 0, to_x).wait_recv()
        if i % 2 == 0:
            go(raw_move(5, chunk, 0, to_y))
        raw_move(1, chunk, 0, to_y).wait_recv()
        if i % 2 == 1:
            go(raw_move(5, chunk, 1, to_x))
    correct(0, to_x)
    correct(1, to_y)

    def relay(i, chunk, forward):
        move(0, chunk, to_x, to_x).wait_recv()
        if i % 2 == 0:
            go(move(5, chunk, to_x, to_y))
        if forward:
            go(move(3, chunk, to_x, sib))
        move(1, chunk, to_y, to_y).wait_recv()
        if i % 2 == 1:
            go(move(5, chunk, to_y, to_x))
        if forward:
            go(move(4, chunk, to_y, sib))

    for i, chunk in enumerate(bulk):
        relay(i, chunk, True)
        if i == 0:
            go(move(3, block, to_x, sib))
            go(move(4, block, to_y, sib))

    @pl.when(core == late)
    def _():
        for chunk in alone:
            move(0, chunk, me, to_x).start()
            move(1, chunk, me, to_y).start()

    for chunk in raws:
        raw_move(5, chunk, 0, to_x).wait_recv()
    small(far_l.at[0], far_l.at[2], 6, to_y).wait_recv()
    small(far_g.at[0], far_g.at[2], 9, to_y).wait_recv()
    correct(2, diag)
    for i, chunk in enumerate(bulk):
        move(5, chunk, diag, to_x).wait_recv()
        go(move(6, chunk, diag, sib))
        if i == 0:
            go(move(6, block, diag, sib))
    arrived = 3 * early + sum(3 * z for _, _, z in bulk) + rows + rows
    all_of(arrived, 2).wait_recv()

    @pl.when(core == late)
    def _():
        for i, chunk in enumerate(alone):
            relay(i, chunk, False)
        for chunk in alone:
            move(5, chunk, diag, to_x).wait_recv()
        all_of(3 * solo, 1).wait_send()
        sum_pair.wait_send()

    @pl.when(core != late)
    def _():
        for c in (sum_x, sum_y, sum_all):
            c.wait_send()

    all_of(3 * sum(z for _, _, z in every), 0).wait_send()
    all_of(arrived, 2).wait_send()
    for c in started:
        c.wait_send()


def tail_kernel(rows, unit, up, after, tail, ready, sent, crossed, recv):
    solo = tail.shape[1]
    me, core, sib, to_x, to_y, diag, flip = place()
    chunks = pairs(0, unit, ALONE)
    whole = (0, solo)
    rest = (to_x, to_y, diag)
    barrier = pltpu.get_barrier_semaphore()

    lanes = {0: 0, 1: 1, 5: 2}

    def remote(src, dst, slot, i, target):
        inner = slot in lanes
        return pltpu.make_async_remote_copy(
            src_ref=src, dst_ref=dst, send_sem=sent.at[0 if inner else 1],
            recv_sem=recv.at[lanes[slot], i] if inner else crossed, device_id={AXIS: target})

    def all_of(out):
        part = tail.at[0:3]
        return pltpu.make_async_remote_copy(
            src_ref=part, dst_ref=part, send_sem=sent.at[out], recv_sem=crossed,
            device_id={AXIS: sib})

    def held(owner, s, z):
        return up.at[pl.ds(pl.multiple_of(owner * rows + rows - solo + s, 8), z), :]

    def move(slot, i, chunk, owner, target, first=False):
        s, z = chunk
        dst = tail.at[owner, s:s + z, :]
        return remote(held(owner, s, z) if first else dst, dst, slot, i, target)

    def copy(owner):
        r = pl.ds(pl.multiple_of(owner * rows + rows - solo, 8), solo)
        tail[owner] = up[r, :]

    def go(c):
        c.start()

    @pl.when(core != late)
    def _():
        for d in (to_x, to_y, sib):
            pl.semaphore_signal(barrier, inc=1, device_id={AXIS: d})
        pl.semaphore_wait(barrier, 2)
        for i, c in enumerate(chunks):
            go(move(0, i, c, me, to_x, True))
            go(move(1, i, c, me, to_y, True))
        for i, c in enumerate(chunks):
            move(0, i, c, to_x, to_x).wait_recv()
            if i % 2 == 0:
                go(move(5, i, c, to_x, to_y))
            move(1, i, c, to_y, to_y).wait_recv()
            if i % 2 == 1:
                go(move(5, i, c, to_y, to_x))
        pl.semaphore_wait(ready, 1)
        go(move(3, 0, whole, to_x, sib))
        go(move(4, 0, whole, to_y, sib))
        for i, c in enumerate(chunks):
            move(5, i, c, diag, to_x).wait_recv()
            go(move(6, i, c, diag, sib))
        all_of(0).wait_send()

    @pl.when(core == late)
    def _():
        pl.semaphore_wait(barrier, 1)
        pl.semaphore_signal(ready, inc=1, device_id={AXIS: sib})
        for i, owner in enumerate(rest):
            go(move(7, i, whole, owner, sib, True))
        for owner in rest:
            copy(owner)

    all_of(1).wait_recv()
    all_of(1).wait_send()


def write_kernel(rows, solo, a_v, b_v, fac, a_hbm, b_hbm, fa_hbm, fb_hbm, done, sem):
    done[...] = jnp.zeros_like(done)
    n = a_v.shape[0] // rows
    first = lax.axis_index(AXIS) // 2 * 2
    waits = [
        pltpu.make_async_copy(fac.at[i, 0], dst, sem.at[i])
        for i, dst in enumerate((fa_hbm, fb_hbm))
    ]
    for c in waits:
        c.start()
    for k in range(n):
        for i, (src, dst) in enumerate(((a_v, a_hbm), (b_v, b_hbm))):
            owner = lax.rem(first + k, n)
            z = rows - solo if i and k > 1 else rows
            r = pl.ds(pl.multiple_of(owner * rows, 8), z)
            pltpu.make_async_copy(src.at[r, :], dst.at[r, :], sem.at[2 + i]).start()
    waits.append(pltpu.make_async_copy(a_v, a_hbm, sem.at[2]))
    r = pl.ds(0, n * rows - (n - 2) * solo)
    waits.append(pltpu.make_async_copy(b_v.at[r, :], b_hbm.at[r, :], sem.at[3]))
    for c in waits:
        c.wait()


def finish_kernel(rows, tail, before, b_hbm, sem):
    n, solo, _ = tail.shape
    first = lax.axis_index(AXIS) // 2 * 2
    for k in range(2, n):
        owner = lax.rem(first + k, n)
        r = pl.ds(pl.multiple_of((owner + 1) * rows - solo, 8), solo)
        pltpu.make_async_copy(tail.at[owner], b_hbm.at[r, :], sem).start()
    part = b_hbm.at[0:(n - 2) * solo, :]
    pltpu.make_async_copy(part, part, sem).wait()


def paired(n, weight_gate, low_gate, high_gate, weight_up, low_up, high_up, norm_gain):
    rows, cols = weight_gate.shape
    unit = rows // 40
    solo = 2 * sum(ALONE) * unit
    early = 2 * sum(RAW) * unit
    full = (n * rows, cols)
    vmem = pl.BlockSpec(memory_space=pltpu.VMEM)
    hbm = pl.BlockSpec(memory_space=pl.ANY)
    space = pl.BlockSpec(memory_space=pltpu.HBM)
    rank = high_gate.shape[0]
    grant = 65472 * 2**10 - (4 * full[0] * cols + 8 * cols) // 2**10 * 2**10 - 24 * 2**10
    moves = 2 * (len(RAW) + len(GATE) + len(UP) + len(ALONE))
    gate, up, fac = pl.pallas_call(
        functools.partial(gather_kernel, unit, solo),
        out_shape=(
            pltpu.VMEM(full, jnp.bfloat16),
            pltpu.VMEM(full, jnp.bfloat16),
            pltpu.VMEM((2, 1, cols), jnp.float32),
        ),
        in_specs=[space] * 7,
        out_specs=(vmem, vmem, vmem),
        scratch_shapes=[
            pltpu.VMEM((2, rows, cols), jnp.bfloat16),
            pltpu.VMEM((2, rank, rows), jnp.bfloat16),
            pltpu.VMEM((2, rank, cols), jnp.bfloat16),
            pltpu.VMEM((1, rows), jnp.float32),
            pltpu.VMEM((2, rows, rank), jnp.bfloat16),
            pltpu.VMEM((2, rows, cols), jnp.float32),
            pltpu.VMEM((rows, 128), jnp.float32),
            pltpu.VMEM((2, 1, cols), jnp.float32),
            pltpu.VMEM((3, 2, 1, cols), jnp.float32),
            pltpu.VMEM((3, 2, 1, cols), jnp.float32),
            pltpu.VMEM((2, 1, cols), jnp.float32),
            pltpu.VMEM((3, early, cols), jnp.bfloat16),
            pltpu.VMEM((3, rank, early), jnp.bfloat16),
            pltpu.VMEM((3, 1, early), jnp.float32),
            pltpu.VMEM((3, early, rank), jnp.bfloat16),
            pltpu.VMEM((3, early, 128), jnp.float32),
            pltpu.SemaphoreType.DMA((7 + 2 * len(RAW),)),
            pltpu.SemaphoreType.DMA((10,)),
            pltpu.SemaphoreType.DMA((10,)),
            pltpu.SemaphoreType.DMA((3,)),
            pltpu.SemaphoreType.DMA,
            pltpu.SemaphoreType.DMA((3, moves)),
        ],
        compiler_params=pltpu.CompilerParams(
            collective_id=0, has_side_effects=True, vmem_limit_bytes=grant
        ),
        name="merge_gather",
    )(weight_gate, weight_up, low_gate.T, low_up.T, high_gate, high_up, norm_gain)
    whole = jax.ShapeDtypeStruct(full, jnp.bfloat16)
    ready_gate, ready_up, factor_gate, factor_up, done = pl.pallas_call(
        functools.partial(write_kernel, rows, solo),
        out_shape=(whole, whole) + (jax.ShapeDtypeStruct((cols,), jnp.float32),) * 2
        + (pltpu.VMEM((8, 128), jnp.float32),),
        in_specs=[vmem, vmem, vmem],
        out_specs=(hbm,) * 4 + (vmem,),
        scratch_shapes=[pltpu.SemaphoreType.DMA((4,))],
        compiler_params=pltpu.CompilerParams(vmem_limit_bytes=2**20),
        name="write_out",
    )(gate, up, fac)
    tail = pl.pallas_call(
        functools.partial(tail_kernel, rows, unit),
        out_shape=pltpu.VMEM((n, solo, cols), jnp.bfloat16),
        in_specs=[vmem, vmem],
        out_specs=vmem,
        scratch_shapes=[
            pltpu.SemaphoreType.REGULAR,
            pltpu.SemaphoreType.DMA((2,)),
            pltpu.SemaphoreType.DMA,
            pltpu.SemaphoreType.DMA((3, 2 * len(ALONE))),
        ],
        compiler_params=pltpu.CompilerParams(
            collective_id=1, has_side_effects=True, vmem_limit_bytes=2**20
        ),
        name="tail_gather",
    )(up, done)
    ready_up = pl.pallas_call(
        functools.partial(finish_kernel, rows),
        out_shape=whole,
        in_specs=[vmem, hbm],
        out_specs=hbm,
        input_output_aliases={1: 0},
        scratch_shapes=[pltpu.SemaphoreType.DMA],
        compiler_params=pltpu.CompilerParams(vmem_limit_bytes=2**20),
        name="finish",
    )(tail, ready_up)
    return ready_gate, ready_up, factor_gate, factor_up


def solution(mesh):
    in_specs = (
        P("shard", "tp"),
        P("shard", None),
        P(None, "tp"),
        P("shard", "tp"),
        P("shard", None),
        P(None, "tp"),
        P("shard"),
    )
    out_specs = (P(None, "tp"), P(None, "tp"), P("tp"), P("tp"))
    n = mesh.shape[AXIS]
    side = math.isqrt(n // 2)
    body = functools.partial(paired, n) if side == 2 and 2 * side * side == n else local
    return jax.shard_map(body, mesh=mesh, in_specs=in_specs, out_specs=out_specs, check_vma=False)
```

```python
import functools
import math

import jax
import jax.numpy as jnp
from jax import lax
from jax.experimental import pallas as pl
from jax.experimental.pallas import tpu as pltpu
from jax.sharding import PartitionSpec as P

mix_rate = 2.0
AXIS = "shard"


def local(weight_gate, low_gate, high_gate, weight_up, low_up, high_up, norm_gain):
    latest_gate = weight_gate.astype(jnp.float32) + mix_rate * jnp.dot(
        low_gate, high_gate, preferred_element_type=jnp.float32
    )
    latest_up = weight_up.astype(jnp.float32) + mix_rate * jnp.dot(
        low_up, high_up, preferred_element_type=jnp.float32
    )
    latest_gained_gate = latest_gate * norm_gain[:, None]
    latest_gained_up = latest_up * norm_gain[:, None]
    total_gate, total_up = lax.psum(
        (
            jnp.sum(latest_gained_gate * latest_gained_gate, axis=0),
            jnp.sum(latest_gained_up * latest_gained_up, axis=0),
        ),
        AXIS,
    )
    factor_gate = jnp.sqrt(total_gate)
    factor_up = jnp.sqrt(total_up)
    narrow_gate = (latest_gained_gate / factor_gate).astype(jnp.bfloat16)
    narrow_up = (latest_gained_up / factor_up).astype(jnp.bfloat16)
    ready_gate = lax.all_gather(narrow_gate, AXIS, axis=0, tiled=True)
    ready_up = lax.all_gather(narrow_up, AXIS, axis=0, tiled=True)
    return (ready_gate, ready_up, factor_gate, factor_up)


late = 0
RAW = (4, 4)
GATE = (12,)
UP = (10,)
ALONE = (7, 3)


def place():
    me = lax.axis_index(AXIS)
    core = lax.rem(me, 2)
    x = lax.rem(me // 2, 2)
    y = me // 4
    to_x = me + 2 - 4 * x
    to_y = me + 4 - 8 * y
    return me, core, me + 1 - 2 * core, to_x, to_y, to_x + 4 - 8 * y, 1 - 2 * core


def pairs(start, unit, sizes):
    out = []
    for z in sizes:
        for _ in range(2):
            out.append((start, z * unit))
            start += z * unit
    return out


def gather_kernel(
    unit, solo, wg_hbm, wu_hbm, lg_hbm, lu_hbm, hg_hbm, hu_hbm, gain_hbm,
    out_g, out_u, fac,
    w_v, l_v, h_v, gain_v, low_v, g_v, col_v, part, mine, heard, rf_v,
    raw_v, far_l, far_g, far_low, far_col,
    in_sem, small_send, small_recv, sent, crossed, recv,
):
    rows, cols = wg_hbm.shape
    me, core, sib, to_x, to_y, diag, flip = place()
    early = 2 * sum(RAW) * unit
    shared_up = rows - solo
    raws = [(0, s, z) for s, z in pairs(0, unit, RAW)]
    bulk = [(0, s, z) for s, z in pairs(early, unit, GATE)]
    bulk += [(1, s, z) for s, z in pairs(0, unit, UP)]
    alone = [(1, s, z) for s, z in pairs(shared_up, unit, ALONE)]
    own_tail = (1, shared_up, solo)
    block = (0, 0, early)
    every = raws + bulk
    order = {c: i for i, c in enumerate(every + alone)}
    lanes = {0: 0, 1: 1, 5: 2}
    outs = (out_g, out_u)

    barrier = pltpu.get_barrier_semaphore()
    for d in (to_x, to_y, sib):
        pl.semaphore_signal(barrier, inc=1, device_id={AXIS: d})

    gain_load = pltpu.make_async_copy(gain_hbm, gain_v.at[0], in_sem.at[6])
    low_loads, high_loads = (
        [
            pltpu.make_async_copy(src, dst.at[a], in_sem.at[3 * a + i])
            for a, src in enumerate(pair)
        ]
        for i, (pair, dst) in enumerate((((lg_hbm, lu_hbm), l_v), ((hg_hbm, hu_hbm), h_v)))
    )
    loads = [
        pltpu.make_async_copy(wg_hbm.at[early:, :], w_v.at[0, early:, :], in_sem.at[2]),
        pltpu.make_async_copy(wu_hbm, w_v.at[1], in_sem.at[5]),
    ]
    raw_loads = [
        pltpu.make_async_copy(wg_hbm.at[s:s + z, :], w_v.at[0, s:s + z, :], in_sem.at[7 + i])
        for i, (_, s, z) in enumerate(raws)
    ]
    for c in raw_loads[:2] + [low_loads[0], gain_load, high_loads[0]] + raw_loads[2:]:
        c.start()
    for c in (loads[0], low_loads[1], high_loads[1], loads[1]):
        c.start()

    started = []

    def keep(c):
        started.append(c)
        c.start()

    def go(c):
        c.start()

    def remote(src, dst, slot, chunk, target):
        if slot in lanes:
            got = recv.at[lanes[slot], order[chunk]]
            out = sent.at[1 if chunk in alone else 0]
        else:
            got, out = crossed, sent.at[2]
        return pltpu.make_async_remote_copy(
            src_ref=src, dst_ref=dst, send_sem=out, recv_sem=got, device_id={AXIS: target})

    def all_of(count, out):
        part = out_g.at[0:count, :]
        return pltpu.make_async_remote_copy(
            src_ref=part, dst_ref=part, send_sem=sent.at[out], recv_sem=crossed,
            device_id={AXIS: sib})

    def small(src, dst, i, target):
        return pltpu.make_async_remote_copy(
            src_ref=src, dst_ref=dst, send_sem=small_send.at[i],
            recv_sem=small_recv.at[i], device_id={AXIS: target})

    def piece(chunk, owner):
        a, s, z = chunk
        return outs[a].at[pl.ds(pl.multiple_of(owner * rows + s, 8), z), :]

    def move(slot, chunk, owner, target):
        p = piece(chunk, owner)
        return remote(p, p, slot, chunk, target)

    def raw_move(slot, chunk, at, target):
        _, s, z = chunk
        src = w_v.at[0, s:s + z, :] if slot < 2 else raw_v.at[at, s:s + z, :]
        return remote(src, raw_v.at[slot if slot < 2 else 2, s:s + z, :], slot, chunk, target)

    pl.semaphore_wait(barrier, 3)
    for c, chunk in list(zip(raw_loads, raws))[:2]:
        c.wait()
        go(raw_move(0, chunk, 0, to_x))
        go(raw_move(1, chunk, 0, to_y))
    low_own, gain_own = l_v.at[0, :, :early], gain_v.at[:, :early]
    low_loads[0].wait()
    gain_load.wait()
    for i, d in enumerate((to_x, to_y)):
        keep(small(low_own, far_l.at[i], 4 + i, d))
        keep(small(gain_own, far_g.at[i], 7 + i, d))

    col_v[...] = jnp.broadcast_to(gain_v[...], (128, rows)).T
    step = rows // 5
    for a in range(2):
        if a:
            low_loads[a].wait()
        else:
            for c in raw_loads[2:]:
                c.wait()
        low_v[a] = (mix_rate * l_v[a].astype(jnp.float32)).T.astype(jnp.bfloat16)
        high_loads[a].wait()
        loads[a].wait()
        acc = jnp.zeros((8, cols), jnp.float32)
        for s in range(0, rows, step):
            r = pl.ds(s, step)
            prod = jnp.dot(low_v[a, r, :], h_v[a], preferred_element_type=jnp.float32)
            new = (w_v[a, r, :].astype(jnp.float32) + prod) * col_v[r, 0:1]
            g_v[a, r, :] = new
            acc = acc + jnp.sum((new * new).reshape(step // 8, 8, cols), axis=0)
        part[a] = jnp.sum(acc, axis=0, keepdims=True)

    sum_pair = small(part, heard.at[0], 0, sib)
    sum_x = small(mine.at[0], heard.at[1], 1, to_x)
    sum_y = small(mine.at[1], heard.at[2], 2, to_y)
    sum_all = small(mine.at[2], mine.at[2], 3, sib)

    @pl.when(core == late)
    def _():
        sum_pair.start()
        for chunk in raws[2:]:
            raw_move(0, chunk, 0, to_x).start()
            raw_move(1, chunk, 0, to_y).start()
        sum_all.wait_recv()

    @pl.when(core != late)
    def _():
        sum_pair.wait_recv()
        mine[0] = part[...] + heard[0]
        raw_move(1, raws[2], 0, to_y).start()
        sum_x.start()
        raw_move(0, raws[2], 0, to_x).start()
        sum_x.wait_recv()
        mine[1] = mine[0] + heard[1]
        raw_move(0, raws[3], 0, to_x).start()
        sum_y.start()
        raw_move(1, raws[3], 0, to_y).start()
        sum_y.wait_recv()
        mine[2] = mine[1] + heard[2]
        sum_all.start()

    for a in range(2):
        factor = jnp.sqrt(mine[2, a])
        fac[a] = factor
        rf_v[a] = 1.0 / factor

    def scale(chunk):
        a, s, z = chunk
        r = pl.ds(pl.multiple_of(me * rows + s, 8), z)
        outs[a][r, :] = (g_v[a, s:s + z, :] * rf_v[a]).astype(jnp.bfloat16)

    def send_own(chunk):
        go(move(0, chunk, me, to_x))
        go(move(1, chunk, me, to_y))
        go(move(2, chunk, me, sib))

    for i, chunk in enumerate(bulk):
        scale(chunk)
        if i:
            send_own(bulk[i - 1])
    scale(block)
    send_own(bulk[-1])
    for chunk in alone:
        scale(chunk)
    go(move(2, block, me, sib))
    go(move(2, own_tail, me, sib))

    low_x, low_y = (small(low_own, far_l.at[i], 4 + i, to_x) for i in range(2))
    gain_x, gain_y = (small(gain_own, far_g.at[i], 7 + i, to_x) for i in range(2))
    low_x.wait_recv()
    keep(small(far_l.at[0], far_l.at[2], 6, to_y))
    gain_x.wait_recv()
    keep(small(far_g.at[0], far_g.at[2], 9, to_y))
    low_y.wait_recv()
    gain_y.wait_recv()

    def correct(i, owner):
        far_low[i] = (mix_rate * far_l[i].astype(jnp.float32)).T.astype(jnp.bfloat16)
        far_col[i] = jnp.broadcast_to(far_g[i], (128, early)).T
        for s in range(0, early, early // 2):
            r = pl.ds(s, early // 2)
            prod = jnp.dot(far_low[i, r, :], h_v[0], preferred_element_type=jnp.float32)
            new = (raw_v[i, r, :].astype(jnp.float32) + prod) * far_col[i, r, 0:1]
            o = pl.ds(pl.multiple_of(owner * rows + s, 8), early // 2)
            out_g[o, :] = (new * rf_v[0]).astype(jnp.bfloat16)

    for i, chunk in enumerate(raws):
        raw_move(0, chunk, 0, to_x).wait_recv()
        if i % 2 == 0:
            go(raw_move(5, chunk, 0, to_y))
        raw_move(1, chunk, 0, to_y).wait_recv()
        if i % 2 == 1:
            go(raw_move(5, chunk, 1, to_x))
    correct(0, to_x)
    correct(1, to_y)

    def relay(i, chunk, forward):
        move(0, chunk, to_x, to_x).wait_recv()
        if i % 2 == 0:
            go(move(5, chunk, to_x, to_y))
        if forward:
            go(move(3, chunk, to_x, sib))
        move(1, chunk, to_y, to_y).wait_recv()
        if i % 2 == 1:
            go(move(5, chunk, to_y, to_x))
        if forward:
            go(move(4, chunk, to_y, sib))

    for i, chunk in enumerate(bulk):
        relay(i, chunk, True)
        if i == 0:
            go(move(3, block, to_x, sib))
            go(move(4, block, to_y, sib))

    @pl.when(core == late)
    def _():
        for chunk in alone:
            move(0, chunk, me, to_x).start()
            move(1, chunk, me, to_y).start()

    for chunk in raws:
        raw_move(5, chunk, 0, to_x).wait_recv()
    small(far_l.at[0], far_l.at[2], 6, to_y).wait_recv()
    small(far_g.at[0], far_g.at[2], 9, to_y).wait_recv()
    correct(2, diag)
    for i, chunk in enumerate(bulk):
        move(5, chunk, diag, to_x).wait_recv()
        go(move(6, chunk, diag, sib))
        if i == 0:
            go(move(6, block, diag, sib))
    arrived = 3 * early + sum(3 * z for _, _, z in bulk) + rows + rows
    all_of(arrived, 2).wait_recv()

    @pl.when(core == late)
    def _():
        for i, chunk in enumerate(alone):
            relay(i, chunk, False)
        for chunk in alone:
            move(5, chunk, diag, to_x).wait_recv()
        all_of(3 * solo, 1).wait_send()
        sum_pair.wait_send()

    @pl.when(core != late)
    def _():
        for c in (sum_x, sum_y, sum_all):
            c.wait_send()

    all_of(3 * sum(z for _, _, z in every), 0).wait_send()
    all_of(arrived, 2).wait_send()
    for c in started:
        c.wait_send()


def tail_kernel(rows, unit, up, after, tail, ready, sent, crossed, recv):
    solo = tail.shape[1]
    me, core, sib, to_x, to_y, diag, flip = place()
    chunks = pairs(0, unit, ALONE)
    whole = (0, solo)
    rest = (to_x, to_y, diag)
    barrier = pltpu.get_barrier_semaphore()

    lanes = {0: 0, 1: 1, 5: 2}

    def remote(src, dst, slot, i, target):
        inner = slot in lanes
        return pltpu.make_async_remote_copy(
            src_ref=src, dst_ref=dst, send_sem=sent.at[0 if inner else 1],
            recv_sem=recv.at[lanes[slot], i] if inner else crossed, device_id={AXIS: target})

    def all_of(out):
        part = tail.at[0:3]
        return pltpu.make_async_remote_copy(
            src_ref=part, dst_ref=part, send_sem=sent.at[out], recv_sem=crossed,
            device_id={AXIS: sib})

    def held(owner, s, z):
        return up.at[pl.ds(pl.multiple_of(owner * rows + rows - solo + s, 8), z), :]

    def move(slot, i, chunk, owner, target, first=False):
        s, z = chunk
        dst = tail.at[owner, s:s + z, :]
        return remote(held(owner, s, z) if first else dst, dst, slot, i, target)

    def go(c):
        c.start()

    @pl.when(core != late)
    def _():
        for d in (to_x, to_y, sib):
            pl.semaphore_signal(barrier, inc=1, device_id={AXIS: d})
        pl.semaphore_wait(barrier, 2)
        for i, c in enumerate(chunks):
            go(move(0, i, c, me, to_x, True))
            go(move(1, i, c, me, to_y, True))
        for i, c in enumerate(chunks):
            move(0, i, c, to_x, to_x).wait_recv()
            if i % 2 == 0:
                go(move(5, i, c, to_x, to_y))
            move(1, i, c, to_y, to_y).wait_recv()
            if i % 2 == 1:
                go(move(5, i, c, to_y, to_x))
        pl.semaphore_wait(ready, 1)
        go(move(3, 0, whole, to_x, sib))
        go(move(4, 0, whole, to_y, sib))
        for i, c in enumerate(chunks):
            move(5, i, c, diag, to_x).wait_recv()
            go(move(6, i, c, diag, sib))
        all_of(0).wait_send()

    @pl.when(core == late)
    def _():
        pl.semaphore_wait(barrier, 1)
        pl.semaphore_signal(ready, inc=1, device_id={AXIS: sib})
        for i, owner in enumerate(rest):
            go(move(7, i, whole, owner, sib, True))

    all_of(1).wait_recv()
    all_of(1).wait_send()


def write_kernel(rows, solo, a_v, b_v, fac, a_hbm, b_hbm, fa_hbm, fb_hbm, done, sem):
    done[...] = jnp.zeros_like(done)
    n = a_v.shape[0] // rows
    first = lax.axis_index(AXIS) // 2 * 2
    waits = [
        pltpu.make_async_copy(fac.at[i, 0], dst, sem.at[i])
        for i, dst in enumerate((fa_hbm, fb_hbm))
    ]
    for c in waits:
        c.start()
    for k in range(n):
        for i, (src, dst) in enumerate(((a_v, a_hbm), (b_v, b_hbm))):
            owner = lax.rem(first + k, n)
            z = rows - solo if i and k > 1 else rows
            r = pl.ds(pl.multiple_of(owner * rows, 8), z)
            pltpu.make_async_copy(src.at[r, :], dst.at[r, :], sem.at[2 + i]).start()
    me = lax.axis_index(AXIS)
    alone = lax.rem(me, 2) == late

    @pl.when(alone)
    def _():
        for k in range(2, n, 2):
            r = pl.ds(pl.multiple_of((lax.rem(me + k, n) + 1) * rows - solo, 8), solo)
            pltpu.make_async_copy(b_v.at[r, :], b_hbm.at[r, :], sem.at[4]).start()

    waits.append(pltpu.make_async_copy(a_v, a_hbm, sem.at[2]))
    r = pl.ds(0, n * rows - (n - 2) * solo)
    waits.append(pltpu.make_async_copy(b_v.at[r, :], b_hbm.at[r, :], sem.at[3]))
    for c in waits:
        c.wait()

    @pl.when(alone)
    def _():
        part = b_hbm.at[0:(n // 2 - 1) * solo, :]
        pltpu.make_async_copy(part, part, sem.at[4]).wait()


def finish_kernel(rows, tail, before, b_hbm, sem):
    n, solo, _ = tail.shape
    me = lax.axis_index(AXIS)
    first = me // 2 * 2
    part = b_hbm.at[0:(n // 2 - 1) * solo, :]

    def write(side):
        for k in range(2, n, 2):
            owner = lax.rem(first + k + side, n)
            r = pl.ds(pl.multiple_of((owner + 1) * rows - solo, 8), solo)
            pltpu.make_async_copy(tail.at[owner], b_hbm.at[r, :], sem.at[side]).start()

    def wait(side):
        pltpu.make_async_copy(part, part, sem.at[side]).wait()

    write(1 - late)
    own = lax.rem(me, 2) == late

    @pl.when(jnp.logical_not(own))
    def _():
        write(late)
        wait(late)

    wait(1 - late)


def paired(n, weight_gate, low_gate, high_gate, weight_up, low_up, high_up, norm_gain):
    rows, cols = weight_gate.shape
    unit = rows // 40
    solo = 2 * sum(ALONE) * unit
    early = 2 * sum(RAW) * unit
    full = (n * rows, cols)
    vmem = pl.BlockSpec(memory_space=pltpu.VMEM)
    hbm = pl.BlockSpec(memory_space=pl.ANY)
    space = pl.BlockSpec(memory_space=pltpu.HBM)
    rank = high_gate.shape[0]
    grant = 65472 * 2**10 - (4 * full[0] * cols + 8 * cols) // 2**10 * 2**10 - 24 * 2**10
    moves = 2 * (len(RAW) + len(GATE) + len(UP) + len(ALONE))
    gate, up, fac = pl.pallas_call(
        functools.partial(gather_kernel, unit, solo),
        out_shape=(
            pltpu.VMEM(full, jnp.bfloat16),
            pltpu.VMEM(full, jnp.bfloat16),
            pltpu.VMEM((2, 1, cols), jnp.float32),
        ),
        in_specs=[space] * 7,
        out_specs=(vmem, vmem, vmem),
        scratch_shapes=[
            pltpu.VMEM((2, rows, cols), jnp.bfloat16),
            pltpu.VMEM((2, rank, rows), jnp.bfloat16),
            pltpu.VMEM((2, rank, cols), jnp.bfloat16),
            pltpu.VMEM((1, rows), jnp.float32),
            pltpu.VMEM((2, rows, rank), jnp.bfloat16),
            pltpu.VMEM((2, rows, cols), jnp.float32),
            pltpu.VMEM((rows, 128), jnp.float32),
            pltpu.VMEM((2, 1, cols), jnp.float32),
            pltpu.VMEM((3, 2, 1, cols), jnp.float32),
            pltpu.VMEM((3, 2, 1, cols), jnp.float32),
            pltpu.VMEM((2, 1, cols), jnp.float32),
            pltpu.VMEM((3, early, cols), jnp.bfloat16),
            pltpu.VMEM((3, rank, early), jnp.bfloat16),
            pltpu.VMEM((3, 1, early), jnp.float32),
            pltpu.VMEM((3, early, rank), jnp.bfloat16),
            pltpu.VMEM((3, early, 128), jnp.float32),
            pltpu.SemaphoreType.DMA((7 + 2 * len(RAW),)),
            pltpu.SemaphoreType.DMA((10,)),
            pltpu.SemaphoreType.DMA((10,)),
            pltpu.SemaphoreType.DMA((3,)),
            pltpu.SemaphoreType.DMA,
            pltpu.SemaphoreType.DMA((3, moves)),
        ],
        compiler_params=pltpu.CompilerParams(
            collective_id=0, has_side_effects=True, vmem_limit_bytes=grant
        ),
        name="merge_gather",
    )(weight_gate, weight_up, low_gate.T, low_up.T, high_gate, high_up, norm_gain)
    whole = jax.ShapeDtypeStruct(full, jnp.bfloat16)
    ready_gate, ready_up, factor_gate, factor_up, done = pl.pallas_call(
        functools.partial(write_kernel, rows, solo),
        out_shape=(whole, whole) + (jax.ShapeDtypeStruct((cols,), jnp.float32),) * 2
        + (pltpu.VMEM((8, 128), jnp.float32),),
        in_specs=[vmem, vmem, vmem],
        out_specs=(hbm,) * 4 + (vmem,),
        scratch_shapes=[pltpu.SemaphoreType.DMA((5,))],
        compiler_params=pltpu.CompilerParams(vmem_limit_bytes=2**20),
        name="write_out",
    )(gate, up, fac)
    tail = pl.pallas_call(
        functools.partial(tail_kernel, rows, unit),
        out_shape=pltpu.VMEM((n, solo, cols), jnp.bfloat16),
        in_specs=[vmem, vmem],
        out_specs=vmem,
        scratch_shapes=[
            pltpu.SemaphoreType.REGULAR,
            pltpu.SemaphoreType.DMA((2,)),
            pltpu.SemaphoreType.DMA,
            pltpu.SemaphoreType.DMA((3, 2 * len(ALONE))),
        ],
        compiler_params=pltpu.CompilerParams(
            collective_id=1, has_side_effects=True, vmem_limit_bytes=2**20
        ),
        name="tail_gather",
    )(up, done)
    ready_up = pl.pallas_call(
        functools.partial(finish_kernel, rows),
        out_shape=whole,
        in_specs=[vmem, hbm],
        out_specs=hbm,
        input_output_aliases={1: 0},
        scratch_shapes=[pltpu.SemaphoreType.DMA((2,))],
        compiler_params=pltpu.CompilerParams(vmem_limit_bytes=2**20),
        name="finish",
    )(tail, ready_up)
    return ready_gate, ready_up, factor_gate, factor_up


def solution(mesh):
    in_specs = (
        P("shard", "tp"),
        P("shard", None),
        P(None, "tp"),
        P("shard", "tp"),
        P("shard", None),
        P(None, "tp"),
        P("shard"),
    )
    out_specs = (P(None, "tp"), P(None, "tp"), P("tp"), P("tp"))
    n = mesh.shape[AXIS]
    side = math.isqrt(n // 2)
    body = functools.partial(paired, n) if side == 2 and 2 * side * side == n else local
    return jax.shard_map(body, mesh=mesh, in_specs=in_specs, out_specs=out_specs, check_vma=False)
```

```python
import functools
import math

import jax
import jax.numpy as jnp
from jax import lax
from jax.experimental import pallas as pl
from jax.experimental.pallas import tpu as pltpu
from jax.sharding import PartitionSpec as P

mix_rate = 2.0
AXIS = "shard"


def local(weight_gate, low_gate, high_gate, weight_up, low_up, high_up, norm_gain):
    latest_gate = weight_gate.astype(jnp.float32) + mix_rate * jnp.dot(
        low_gate, high_gate, preferred_element_type=jnp.float32
    )
    latest_up = weight_up.astype(jnp.float32) + mix_rate * jnp.dot(
        low_up, high_up, preferred_element_type=jnp.float32
    )
    latest_gained_gate = latest_gate * norm_gain[:, None]
    latest_gained_up = latest_up * norm_gain[:, None]
    total_gate, total_up = lax.psum(
        (
            jnp.sum(latest_gained_gate * latest_gained_gate, axis=0),
            jnp.sum(latest_gained_up * latest_gained_up, axis=0),
        ),
        AXIS,
    )
    factor_gate = jnp.sqrt(total_gate)
    factor_up = jnp.sqrt(total_up)
    narrow_gate = (latest_gained_gate / factor_gate).astype(jnp.bfloat16)
    narrow_up = (latest_gained_up / factor_up).astype(jnp.bfloat16)
    ready_gate = lax.all_gather(narrow_gate, AXIS, axis=0, tiled=True)
    ready_up = lax.all_gather(narrow_up, AXIS, axis=0, tiled=True)
    return (ready_gate, ready_up, factor_gate, factor_up)


late = 0
RAW = (4, 4)
GATE = (12,)
UP = (10,)
ALONE = (5, 3, 2)


def place():
    me = lax.axis_index(AXIS)
    core = lax.rem(me, 2)
    x = lax.rem(me // 2, 2)
    y = me // 4
    to_x = me + 2 - 4 * x
    to_y = me + 4 - 8 * y
    return me, core, me + 1 - 2 * core, to_x, to_y, to_x + 4 - 8 * y, 1 - 2 * core


def pairs(start, unit, sizes):
    out = []
    for z in sizes:
        for _ in range(2):
            out.append((start, z * unit))
            start += z * unit
    return out


def gather_kernel(
    unit, solo, wg_hbm, wu_hbm, lg_hbm, lu_hbm, hg_hbm, hu_hbm, gain_hbm,
    out_g, out_u, fac,
    w_v, l_v, h_v, gain_v, low_v, g_v, col_v, part, mine, heard, rf_v,
    raw_v, far_l, far_g, far_low, far_col,
    in_sem, small_send, small_recv, sent, crossed, recv,
):
    rows, cols = wg_hbm.shape
    me, core, sib, to_x, to_y, diag, flip = place()
    early = 2 * sum(RAW) * unit
    shared_up = rows - solo
    raws = [(0, s, z) for s, z in pairs(0, unit, RAW)]
    bulk = [(0, s, z) for s, z in pairs(early, unit, GATE)]
    bulk += [(1, s, z) for s, z in pairs(0, unit, UP)]
    alone = [(1, s, z) for s, z in pairs(shared_up, unit, ALONE)]
    own_tail = (1, shared_up, solo)
    block = (0, 0, early)
    every = raws + bulk
    order = {c: i for i, c in enumerate(every + alone)}
    lanes = {0: 0, 1: 1, 5: 2}
    outs = (out_g, out_u)

    barrier = pltpu.get_barrier_semaphore()
    for d in (to_x, to_y, sib):
        pl.semaphore_signal(barrier, inc=1, device_id={AXIS: d})

    gain_load = pltpu.make_async_copy(gain_hbm, gain_v.at[0], in_sem.at[6])
    low_loads, high_loads = (
        [
            pltpu.make_async_copy(src, dst.at[a], in_sem.at[3 * a + i])
            for a, src in enumerate(pair)
        ]
        for i, (pair, dst) in enumerate((((lg_hbm, lu_hbm), l_v), ((hg_hbm, hu_hbm), h_v)))
    )
    loads = [
        pltpu.make_async_copy(wg_hbm.at[early:, :], w_v.at[0, early:, :], in_sem.at[2]),
        pltpu.make_async_copy(wu_hbm, w_v.at[1], in_sem.at[5]),
    ]
    raw_loads = [
        pltpu.make_async_copy(wg_hbm.at[s:s + z, :], w_v.at[0, s:s + z, :], in_sem.at[7 + i])
        for i, (_, s, z) in enumerate(raws)
    ]
    for c in raw_loads[:2] + [low_loads[0], gain_load, high_loads[0]] + raw_loads[2:]:
        c.start()
    for c in (loads[0], low_loads[1], high_loads[1], loads[1]):
        c.start()

    started = []

    def keep(c):
        started.append(c)
        c.start()

    def go(c):
        c.start()

    def remote(src, dst, slot, chunk, target):
        if slot in lanes:
            got = recv.at[lanes[slot], order[chunk]]
            out = sent.at[1 if chunk in alone else 0]
        else:
            got, out = crossed, sent.at[2]
        return pltpu.make_async_remote_copy(
            src_ref=src, dst_ref=dst, send_sem=out, recv_sem=got, device_id={AXIS: target})

    def all_of(count, out):
        part = out_g.at[0:count, :]
        return pltpu.make_async_remote_copy(
            src_ref=part, dst_ref=part, send_sem=sent.at[out], recv_sem=crossed,
            device_id={AXIS: sib})

    def small(src, dst, i, target):
        return pltpu.make_async_remote_copy(
            src_ref=src, dst_ref=dst, send_sem=small_send.at[i],
            recv_sem=small_recv.at[i], device_id={AXIS: target})

    def piece(chunk, owner):
        a, s, z = chunk
        return outs[a].at[pl.ds(pl.multiple_of(owner * rows + s, 8), z), :]

    def move(slot, chunk, owner, target):
        p = piece(chunk, owner)
        return remote(p, p, slot, chunk, target)

    def raw_move(slot, chunk, at, target):
        _, s, z = chunk
        src = w_v.at[0, s:s + z, :] if slot < 2 else raw_v.at[at, s:s + z, :]
        return remote(src, raw_v.at[slot if slot < 2 else 2, s:s + z, :], slot, chunk, target)

    pl.semaphore_wait(barrier, 3)
    for c, chunk in list(zip(raw_loads, raws))[:2]:
        c.wait()
        go(raw_move(0, chunk, 0, to_x))
        go(raw_move(1, chunk, 0, to_y))
    low_own, gain_own = l_v.at[0, :, :early], gain_v.at[:, :early]
    low_loads[0].wait()
    gain_load.wait()
    for i, d in enumerate((to_x, to_y)):
        keep(small(low_own, far_l.at[i], 4 + i, d))
        keep(small(gain_own, far_g.at[i], 7 + i, d))

    col_v[...] = jnp.broadcast_to(gain_v[...], (128, rows)).T
    step = rows // 5
    for a in range(2):
        if a:
            low_loads[a].wait()
        else:
            for c in raw_loads[2:]:
                c.wait()
        low_v[a] = (mix_rate * l_v[a].astype(jnp.float32)).T.astype(jnp.bfloat16)
        high_loads[a].wait()
        loads[a].wait()
        acc = jnp.zeros((8, cols), jnp.float32)
        for s in range(0, rows, step):
            r = pl.ds(s, step)
            prod = jnp.dot(low_v[a, r, :], h_v[a], preferred_element_type=jnp.float32)
            new = (w_v[a, r, :].astype(jnp.float32) + prod) * col_v[r, 0:1]
            g_v[a, r, :] = new
            acc = acc + jnp.sum((new * new).reshape(step // 8, 8, cols), axis=0)
        part[a] = jnp.sum(acc, axis=0, keepdims=True)

    sum_pair = small(part, heard.at[0], 0, sib)
    sum_x = small(mine.at[0], heard.at[1], 1, to_x)
    sum_y = small(mine.at[1], heard.at[2], 2, to_y)
    sum_all = small(mine.at[2], mine.at[2], 3, sib)

    @pl.when(core == late)
    def _():
        sum_pair.start()
        for chunk in raws[2:]:
            raw_move(0, chunk, 0, to_x).start()
            raw_move(1, chunk, 0, to_y).start()
        sum_all.wait_recv()

    @pl.when(core != late)
    def _():
        sum_pair.wait_recv()
        mine[0] = part[...] + heard[0]
        raw_move(1, raws[2], 0, to_y).start()
        sum_x.start()
        raw_move(0, raws[2], 0, to_x).start()
        sum_x.wait_recv()
        mine[1] = mine[0] + heard[1]
        raw_move(0, raws[3], 0, to_x).start()
        sum_y.start()
        raw_move(1, raws[3], 0, to_y).start()
        sum_y.wait_recv()
        mine[2] = mine[1] + heard[2]
        sum_all.start()

    for a in range(2):
        factor = jnp.sqrt(mine[2, a])
        fac[a] = factor
        rf_v[a] = 1.0 / factor

    def scale(chunk):
        a, s, z = chunk
        r = pl.ds(pl.multiple_of(me * rows + s, 8), z)
        outs[a][r, :] = (g_v[a, s:s + z, :] * rf_v[a]).astype(jnp.bfloat16)

    def send_own(chunk):
        go(move(0, chunk, me, to_x))
        go(move(1, chunk, me, to_y))
        go(move(2, chunk, me, sib))

    for i, chunk in enumerate(bulk):
        scale(chunk)
        if i:
            send_own(bulk[i - 1])
    scale(block)
    send_own(bulk[-1])
    for chunk in alone:
        scale(chunk)
    go(move(2, block, me, sib))
    go(move(2, own_tail, me, sib))

    low_x, low_y = (small(low_own, far_l.at[i], 4 + i, to_x) for i in range(2))
    gain_x, gain_y = (small(gain_own, far_g.at[i], 7 + i, to_x) for i in range(2))
    for c in (low_x, low_y, gain_x, gain_y):
        c.wait_recv()
    over = to_y + core * (to_x - to_y)
    keep(small(far_l.at[core], far_l.at[2], 6, over))
    keep(small(far_g.at[core], far_g.at[2], 9, over))

    def correct(i, owner):
        far_low[i] = (mix_rate * far_l[i].astype(jnp.float32)).T.astype(jnp.bfloat16)
        far_col[i] = jnp.broadcast_to(far_g[i], (128, early)).T
        for s in range(0, early, early // 2):
            r = pl.ds(s, early // 2)
            prod = jnp.dot(far_low[i, r, :], h_v[0], preferred_element_type=jnp.float32)
            new = (raw_v[i, r, :].astype(jnp.float32) + prod) * far_col[i, r, 0:1]
            o = pl.ds(pl.multiple_of(owner * rows + s, 8), early // 2)
            out_g[o, :] = (new * rf_v[0]).astype(jnp.bfloat16)

    for i, chunk in enumerate(raws):
        raw_move(0, chunk, 0, to_x).wait_recv()
        if i % 2 == 0:
            go(raw_move(5, chunk, 0, to_y))
        raw_move(1, chunk, 0, to_y).wait_recv()
        if i % 2 == 1:
            go(raw_move(5, chunk, 1, to_x))
    correct(0, to_x)
    correct(1, to_y)

    def relay(i, chunk, forward):
        move(0, chunk, to_x, to_x).wait_recv()
        if i % 2 == 0:
            go(move(5, chunk, to_x, to_y))
        if forward:
            go(move(3, chunk, to_x, sib))
        move(1, chunk, to_y, to_y).wait_recv()
        if i % 2 == 1:
            go(move(5, chunk, to_y, to_x))
        if forward:
            go(move(4, chunk, to_y, sib))

    for i, chunk in enumerate(bulk):
        relay(i, chunk, True)
        if i == 0:
            go(move(3, block, to_x, sib))
            go(move(4, block, to_y, sib))

    @pl.when(core == late)
    def _():
        for chunk in alone:
            move(0, chunk, me, to_x).start()
            move(1, chunk, me, to_y).start()

    for chunk in raws:
        raw_move(5, chunk, 0, to_x).wait_recv()
    small(far_l.at[0], far_l.at[2], 6, to_y).wait_recv()
    small(far_g.at[0], far_g.at[2], 9, to_y).wait_recv()
    correct(2, diag)
    for i, chunk in enumerate(bulk):
        move(5, chunk, diag, to_x).wait_recv()
        go(move(6, chunk, diag, sib))
        if i == 0:
            go(move(6, block, diag, sib))
    arrived = 3 * early + sum(3 * z for _, _, z in bulk) + rows + rows
    all_of(arrived, 2).wait_recv()

    @pl.when(core == late)
    def _():
        for i, chunk in enumerate(alone):
            relay(i, chunk, False)
        for chunk in alone:
            move(5, chunk, diag, to_x).wait_recv()
        all_of(3 * solo, 1).wait_send()
        sum_pair.wait_send()

    @pl.when(core != late)
    def _():
        for c in (sum_x, sum_y, sum_all):
            c.wait_send()

    all_of(3 * sum(z for _, _, z in every), 0).wait_send()
    all_of(arrived, 2).wait_send()
    for c in started:
        c.wait_send()


def tail_kernel(rows, unit, up, after, tail, ready, sent, crossed, recv):
    solo = tail.shape[1]
    me, core, sib, to_x, to_y, diag, flip = place()
    chunks = pairs(0, unit, ALONE)
    whole = (0, solo)
    rest = (to_x, to_y, diag)
    barrier = pltpu.get_barrier_semaphore()

    lanes = {0: 0, 1: 1, 5: 2}

    def remote(src, dst, slot, i, target):
        inner = slot in lanes
        return pltpu.make_async_remote_copy(
            src_ref=src, dst_ref=dst, send_sem=sent.at[0 if inner else 1],
            recv_sem=recv.at[lanes[slot], i] if inner else crossed, device_id={AXIS: target})

    def all_of(out):
        part = tail.at[0:3]
        return pltpu.make_async_remote_copy(
            src_ref=part, dst_ref=part, send_sem=sent.at[out], recv_sem=crossed,
            device_id={AXIS: sib})

    def held(owner, s, z):
        return up.at[pl.ds(pl.multiple_of(owner * rows + rows - solo + s, 8), z), :]

    def move(slot, i, chunk, owner, target, first=False):
        s, z = chunk
        dst = tail.at[owner, s:s + z, :]
        return remote(held(owner, s, z) if first else dst, dst, slot, i, target)

    def go(c):
        c.start()

    @pl.when(core != late)
    def _():
        for d in (to_x, to_y, sib):
            pl.semaphore_signal(barrier, inc=1, device_id={AXIS: d})
        pl.semaphore_wait(barrier, 2)
        for i, c in enumerate(chunks):
            go(move(0, i, c, me, to_x, True))
            go(move(1, i, c, me, to_y, True))
        for i, c in enumerate(chunks):
            move(0, i, c, to_x, to_x).wait_recv()
            if i % 2 == 0:
                go(move(5, i, c, to_x, to_y))
            move(1, i, c, to_y, to_y).wait_recv()
            if i % 2 == 1:
                go(move(5, i, c, to_y, to_x))
        pl.semaphore_wait(ready, 1)
        go(move(3, 0, whole, to_x, sib))
        go(move(4, 0, whole, to_y, sib))
        for i, c in enumerate(chunks):
            move(5, i, c, diag, to_x).wait_recv()
            go(move(6, i, c, diag, sib))
        all_of(0).wait_send()

    @pl.when(core == late)
    def _():
        pl.semaphore_wait(barrier, 1)
        pl.semaphore_signal(ready, inc=1, device_id={AXIS: sib})
        for i, owner in enumerate(rest):
            go(move(7, i, whole, owner, sib, True))

    all_of(1).wait_recv()
    all_of(1).wait_send()


def write_kernel(rows, solo, a_v, b_v, fac, a_hbm, b_hbm, fa_hbm, fb_hbm, done, sem):
    done[...] = jnp.zeros_like(done)
    n = a_v.shape[0] // rows
    first = lax.axis_index(AXIS) // 2 * 2
    waits = [
        pltpu.make_async_copy(fac.at[i, 0], dst, sem.at[i])
        for i, dst in enumerate((fa_hbm, fb_hbm))
    ]
    for c in waits:
        c.start()
    for k in range(n):
        for i, (src, dst) in enumerate(((a_v, a_hbm), (b_v, b_hbm))):
            owner = lax.rem(first + k, n)
            z = rows - solo if i and k > 1 else rows
            r = pl.ds(pl.multiple_of(owner * rows, 8), z)
            pltpu.make_async_copy(src.at[r, :], dst.at[r, :], sem.at[2 + i]).start()
    me = lax.axis_index(AXIS)
    alone = lax.rem(me, 2) == late

    @pl.when(alone)
    def _():
        for k in range(2, n, 2):
            r = pl.ds(pl.multiple_of((lax.rem(me + k, n) + 1) * rows - solo, 8), solo)
            pltpu.make_async_copy(b_v.at[r, :], b_hbm.at[r, :], sem.at[4]).start()

    waits.append(pltpu.make_async_copy(a_v, a_hbm, sem.at[2]))
    r = pl.ds(0, n * rows - (n - 2) * solo)
    waits.append(pltpu.make_async_copy(b_v.at[r, :], b_hbm.at[r, :], sem.at[3]))
    for c in waits:
        c.wait()

    @pl.when(alone)
    def _():
        part = b_hbm.at[0:(n // 2 - 1) * solo, :]
        pltpu.make_async_copy(part, part, sem.at[4]).wait()


def finish_kernel(rows, tail, before, b_hbm, sem):
    n, solo, _ = tail.shape
    me = lax.axis_index(AXIS)
    first = me // 2 * 2
    part = b_hbm.at[0:(n // 2 - 1) * solo, :]

    def write(side):
        for k in range(2, n, 2):
            owner = lax.rem(first + k + side, n)
            r = pl.ds(pl.multiple_of((owner + 1) * rows - solo, 8), solo)
            pltpu.make_async_copy(tail.at[owner], b_hbm.at[r, :], sem.at[side]).start()

    def wait(side):
        pltpu.make_async_copy(part, part, sem.at[side]).wait()

    write(1 - late)
    own = lax.rem(me, 2) == late

    @pl.when(jnp.logical_not(own))
    def _():
        write(late)
        wait(late)

    wait(1 - late)


def paired(n, weight_gate, low_gate, high_gate, weight_up, low_up, high_up, norm_gain):
    rows, cols = weight_gate.shape
    unit = rows // 40
    solo = 2 * sum(ALONE) * unit
    early = 2 * sum(RAW) * unit
    full = (n * rows, cols)
    vmem = pl.BlockSpec(memory_space=pltpu.VMEM)
    hbm = pl.BlockSpec(memory_space=pl.ANY)
    space = pl.BlockSpec(memory_space=pltpu.HBM)
    rank = high_gate.shape[0]
    grant = 65472 * 2**10 - (4 * full[0] * cols + 8 * cols) // 2**10 * 2**10 - 24 * 2**10
    moves = 2 * (len(RAW) + len(GATE) + len(UP) + len(ALONE))
    gate, up, fac = pl.pallas_call(
        functools.partial(gather_kernel, unit, solo),
        out_shape=(
            pltpu.VMEM(full, jnp.bfloat16),
            pltpu.VMEM(full, jnp.bfloat16),
            pltpu.VMEM((2, 1, cols), jnp.float32),
        ),
        in_specs=[space] * 7,
        out_specs=(vmem, vmem, vmem),
        scratch_shapes=[
            pltpu.VMEM((2, rows, cols), jnp.bfloat16),
            pltpu.VMEM((2, rank, rows), jnp.bfloat16),
            pltpu.VMEM((2, rank, cols), jnp.bfloat16),
            pltpu.VMEM((1, rows), jnp.float32),
            pltpu.VMEM((2, rows, rank), jnp.bfloat16),
            pltpu.VMEM((2, rows, cols), jnp.float32),
            pltpu.VMEM((rows, 128), jnp.float32),
            pltpu.VMEM((2, 1, cols), jnp.float32),
            pltpu.VMEM((3, 2, 1, cols), jnp.float32),
            pltpu.VMEM((3, 2, 1, cols), jnp.float32),
            pltpu.VMEM((2, 1, cols), jnp.float32),
            pltpu.VMEM((3, early, cols), jnp.bfloat16),
            pltpu.VMEM((3, rank, early), jnp.bfloat16),
            pltpu.VMEM((3, 1, early), jnp.float32),
            pltpu.VMEM((3, early, rank), jnp.bfloat16),
            pltpu.VMEM((3, early, 128), jnp.float32),
            pltpu.SemaphoreType.DMA((7 + 2 * len(RAW),)),
            pltpu.SemaphoreType.DMA((10,)),
            pltpu.SemaphoreType.DMA((10,)),
            pltpu.SemaphoreType.DMA((3,)),
            pltpu.SemaphoreType.DMA,
            pltpu.SemaphoreType.DMA((3, moves)),
        ],
        compiler_params=pltpu.CompilerParams(
            collective_id=0, has_side_effects=True, vmem_limit_bytes=grant
        ),
        name="merge_gather",
    )(weight_gate, weight_up, low_gate.T, low_up.T, high_gate, high_up, norm_gain)
    whole = jax.ShapeDtypeStruct(full, jnp.bfloat16)
    ready_gate, ready_up, factor_gate, factor_up, done = pl.pallas_call(
        functools.partial(write_kernel, rows, solo),
        out_shape=(whole, whole) + (jax.ShapeDtypeStruct((cols,), jnp.float32),) * 2
        + (pltpu.VMEM((8, 128), jnp.float32),),
        in_specs=[vmem, vmem, vmem],
        out_specs=(hbm,) * 4 + (vmem,),
        scratch_shapes=[pltpu.SemaphoreType.DMA((5,))],
        compiler_params=pltpu.CompilerParams(vmem_limit_bytes=2**20),
        name="write_out",
    )(gate, up, fac)
    tail = pl.pallas_call(
        functools.partial(tail_kernel, rows, unit),
        out_shape=pltpu.VMEM((n, solo, cols), jnp.bfloat16),
        in_specs=[vmem, vmem],
        out_specs=vmem,
        scratch_shapes=[
            pltpu.SemaphoreType.REGULAR,
            pltpu.SemaphoreType.DMA((2,)),
            pltpu.SemaphoreType.DMA,
            pltpu.SemaphoreType.DMA((3, 2 * len(ALONE))),
        ],
        compiler_params=pltpu.CompilerParams(
            collective_id=1, has_side_effects=True, vmem_limit_bytes=2**20
        ),
        name="tail_gather",
    )(up, done)
    ready_up = pl.pallas_call(
        functools.partial(finish_kernel, rows),
        out_shape=whole,
        in_specs=[vmem, hbm],
        out_specs=hbm,
        input_output_aliases={1: 0},
        scratch_shapes=[pltpu.SemaphoreType.DMA((2,))],
        compiler_params=pltpu.CompilerParams(vmem_limit_bytes=2**20),
        name="finish",
    )(tail, ready_up)
    return ready_gate, ready_up, factor_gate, factor_up


def solution(mesh):
    in_specs = (
        P("shard", "tp"),
        P("shard", None),
        P(None, "tp"),
        P("shard", "tp"),
        P("shard", None),
        P(None, "tp"),
        P("shard"),
    )
    out_specs = (P(None, "tp"), P(None, "tp"), P("tp"), P("tp"))
    n = mesh.shape[AXIS]
    side = math.isqrt(n // 2)
    body = functools.partial(paired, n) if side == 2 and 2 * side * side == n else local
    return jax.shard_map(body, mesh=mesh, in_specs=in_specs, out_specs=out_specs, check_vma=False)
```

```python
import functools
import math

import jax
import jax.numpy as jnp
from jax import lax
from jax.experimental import pallas as pl
from jax.experimental.pallas import tpu as pltpu
from jax.sharding import PartitionSpec as P

mix_rate = 2.0
AXIS = "shard"


def local(weight_gate, low_gate, high_gate, weight_up, low_up, high_up, norm_gain):
    latest_gate = weight_gate.astype(jnp.float32) + mix_rate * jnp.dot(
        low_gate, high_gate, preferred_element_type=jnp.float32
    )
    latest_up = weight_up.astype(jnp.float32) + mix_rate * jnp.dot(
        low_up, high_up, preferred_element_type=jnp.float32
    )
    latest_gained_gate = latest_gate * norm_gain[:, None]
    latest_gained_up = latest_up * norm_gain[:, None]
    total_gate, total_up = lax.psum(
        (
            jnp.sum(latest_gained_gate * latest_gained_gate, axis=0),
            jnp.sum(latest_gained_up * latest_gained_up, axis=0),
        ),
        AXIS,
    )
    factor_gate = jnp.sqrt(total_gate)
    factor_up = jnp.sqrt(total_up)
    narrow_gate = (latest_gained_gate / factor_gate).astype(jnp.bfloat16)
    narrow_up = (latest_gained_up / factor_up).astype(jnp.bfloat16)
    ready_gate = lax.all_gather(narrow_gate, AXIS, axis=0, tiled=True)
    ready_up = lax.all_gather(narrow_up, AXIS, axis=0, tiled=True)
    return (ready_gate, ready_up, factor_gate, factor_up)


late = 0
RAW = (2, 6)
GATE = (12,)
UP = (10,)
ALONE = (5, 3, 2)


def place():
    me = lax.axis_index(AXIS)
    core = lax.rem(me, 2)
    x = lax.rem(me // 2, 2)
    y = me // 4
    to_x = me + 2 - 4 * x
    to_y = me + 4 - 8 * y
    return me, core, me + 1 - 2 * core, to_x, to_y, to_x + 4 - 8 * y, 1 - 2 * core


def pairs(start, unit, sizes):
    out = []
    for z in sizes:
        for _ in range(2):
            out.append((start, z * unit))
            start += z * unit
    return out


def gather_kernel(
    unit, solo, wg_hbm, wu_hbm, lg_hbm, lu_hbm, hg_hbm, hu_hbm, gain_hbm,
    out_g, out_u, fac,
    w_v, l_v, h_v, gain_v, low_v, g_v, col_v, part, mine, heard, rf_v,
    raw_v, far_l, far_g, far_low, far_col,
    in_sem, small_send, small_recv, sent, crossed, recv,
):
    rows, cols = wg_hbm.shape
    me, core, sib, to_x, to_y, diag, flip = place()
    early = 2 * sum(RAW) * unit
    shared_up = rows - solo
    raws = [(0, s, z) for s, z in pairs(0, unit, RAW)]
    bulk = [(0, s, z) for s, z in pairs(early, unit, GATE)]
    bulk += [(1, s, z) for s, z in pairs(0, unit, UP)]
    alone = [(1, s, z) for s, z in pairs(shared_up, unit, ALONE)]
    own_tail = (1, shared_up, solo)
    block = (0, 0, early)
    every = raws + bulk
    order = {c: i for i, c in enumerate(every + alone)}
    lanes = {0: 0, 1: 1, 5: 2}
    outs = (out_g, out_u)

    barrier = pltpu.get_barrier_semaphore()
    for d in (to_x, to_y, sib):
        pl.semaphore_signal(barrier, inc=1, device_id={AXIS: d})

    gain_load = pltpu.make_async_copy(gain_hbm, gain_v.at[0], in_sem.at[6])
    low_loads, high_loads = (
        [
            pltpu.make_async_copy(src, dst.at[a], in_sem.at[3 * a + i])
            for a, src in enumerate(pair)
        ]
        for i, (pair, dst) in enumerate((((lg_hbm, lu_hbm), l_v), ((hg_hbm, hu_hbm), h_v)))
    )
    loads = [
        pltpu.make_async_copy(wg_hbm.at[early:, :], w_v.at[0, early:, :], in_sem.at[2]),
        pltpu.make_async_copy(wu_hbm, w_v.at[1], in_sem.at[5]),
    ]
    raw_loads = [
        pltpu.make_async_copy(wg_hbm.at[s:s + z, :], w_v.at[0, s:s + z, :], in_sem.at[7 + i])
        for i, (_, s, z) in enumerate(raws)
    ]
    for c in raw_loads[:2] + [low_loads[0], gain_load, high_loads[0]] + raw_loads[2:]:
        c.start()
    for c in (loads[0], low_loads[1], high_loads[1], loads[1]):
        c.start()

    def go(c):
        c.start()

    def remote(src, dst, slot, chunk, target):
        if slot in lanes:
            got = recv.at[lanes[slot], order[chunk]]
            out = sent.at[1 if chunk in alone else 0]
        else:
            got, out = crossed, sent.at[2]
        return pltpu.make_async_remote_copy(
            src_ref=src, dst_ref=dst, send_sem=out, recv_sem=got, device_id={AXIS: target})

    def all_of(count, out):
        part = out_g.at[0:count, :]
        return pltpu.make_async_remote_copy(
            src_ref=part, dst_ref=part, send_sem=sent.at[out], recv_sem=crossed,
            device_id={AXIS: sib})

    def small(src, dst, i, target):
        return pltpu.make_async_remote_copy(
            src_ref=src, dst_ref=dst, send_sem=small_send.at[(i >= 4) + (i >= 7)],
            recv_sem=small_recv.at[i], device_id={AXIS: target})

    def piece(chunk, owner):
        a, s, z = chunk
        return outs[a].at[pl.ds(pl.multiple_of(owner * rows + s, 8), z), :]

    def move(slot, chunk, owner, target):
        p = piece(chunk, owner)
        return remote(p, p, slot, chunk, target)

    def raw_move(slot, chunk, at, target):
        _, s, z = chunk
        src = w_v.at[0, s:s + z, :] if slot < 2 else raw_v.at[at, s:s + z, :]
        return remote(src, raw_v.at[slot if slot < 2 else 2, s:s + z, :], slot, chunk, target)

    pl.semaphore_wait(barrier, 3)
    for c, chunk in list(zip(raw_loads, raws))[:2]:
        c.wait()
        go(raw_move(0, chunk, 0, to_x))
        go(raw_move(1, chunk, 0, to_y))
    low_own, gain_own = l_v.at[0, :, :early], gain_v.at[:, :early]
    low_loads[0].wait()
    gain_load.wait()
    for i, d in enumerate((to_x, to_y)):
        go(small(low_own, far_l.at[i], 4 + i, d))
        go(small(gain_own, far_g.at[i], 7 + i, d))

    col_v[...] = jnp.broadcast_to(gain_v[...], (128, rows)).T
    step = rows // 5
    for a in range(2):
        if a:
            low_loads[a].wait()
        else:
            for c in raw_loads[2:]:
                c.wait()
        low_v[a] = (mix_rate * l_v[a].astype(jnp.float32)).T.astype(jnp.bfloat16)
        high_loads[a].wait()
        loads[a].wait()
        acc = jnp.zeros((8, cols), jnp.float32)
        for s in range(0, rows, step):
            r = pl.ds(s, step)
            prod = jnp.dot(low_v[a, r, :], h_v[a], preferred_element_type=jnp.float32)
            new = (w_v[a, r, :].astype(jnp.float32) + prod) * col_v[r, 0:1]
            g_v[a, r, :] = new
            acc = acc + jnp.sum((new * new).reshape(step // 8, 8, cols), axis=0)
        part[a] = jnp.sum(acc, axis=0, keepdims=True)

    sum_pair = small(part, heard.at[0], 0, sib)
    sum_x = small(mine.at[0], heard.at[1], 1, to_x)
    sum_y = small(mine.at[1], heard.at[2], 2, to_y)
    sum_all = small(mine.at[2], mine.at[2], 3, sib)

    @pl.when(core == late)
    def _():
        sum_pair.start()
        for chunk in raws[2:]:
            raw_move(0, chunk, 0, to_x).start()
            raw_move(1, chunk, 0, to_y).start()
        sum_all.wait_recv()

    @pl.when(core != late)
    def _():
        sum_pair.wait_recv()
        mine[0] = part[...] + heard[0]
        raw_move(1, raws[2], 0, to_y).start()
        sum_x.start()
        raw_move(0, raws[2], 0, to_x).start()
        sum_x.wait_recv()
        mine[1] = mine[0] + heard[1]
        raw_move(0, raws[3], 0, to_x).start()
        sum_y.start()
        raw_move(1, raws[3], 0, to_y).start()
        sum_y.wait_recv()
        mine[2] = mine[1] + heard[2]
        sum_all.start()

    for a in range(2):
        factor = jnp.sqrt(mine[2, a])
        fac[a] = factor
        rf_v[a] = 1.0 / factor

    def scale(chunk):
        a, s, z = chunk
        r = pl.ds(pl.multiple_of(me * rows + s, 8), z)
        outs[a][r, :] = (g_v[a, s:s + z, :] * rf_v[a]).astype(jnp.bfloat16)

    def send_own(chunk):
        go(move(0, chunk, me, to_x))
        go(move(1, chunk, me, to_y))
        go(move(2, chunk, me, sib))

    for i, chunk in enumerate(bulk):
        scale(chunk)
        if i:
            send_own(bulk[i - 1])
    scale(block)
    send_own(bulk[-1])
    for chunk in alone:
        scale(chunk)
    go(move(2, block, me, sib))
    go(move(2, own_tail, me, sib))

    low_x, low_y = (small(low_own, far_l.at[i], 4 + i, to_x) for i in range(2))
    gain_x, gain_y = (small(gain_own, far_g.at[i], 7 + i, to_x) for i in range(2))
    for c in (low_x, low_y, gain_x, gain_y):
        c.wait_recv()
    over = to_y + core * (to_x - to_y)
    go(small(far_l.at[core], far_l.at[2], 6, over))
    go(small(far_g.at[core], far_g.at[2], 9, over))

    def correct(i, owner):
        far_low[i] = (mix_rate * far_l[i].astype(jnp.float32)).T.astype(jnp.bfloat16)
        far_col[i] = jnp.broadcast_to(far_g[i], (128, early)).T
        for s in range(0, early, early // 2):
            r = pl.ds(s, early // 2)
            prod = jnp.dot(far_low[i, r, :], h_v[0], preferred_element_type=jnp.float32)
            new = (raw_v[i, r, :].astype(jnp.float32) + prod) * far_col[i, r, 0:1]
            o = pl.ds(pl.multiple_of(owner * rows + s, 8), early // 2)
            out_g[o, :] = (new * rf_v[0]).astype(jnp.bfloat16)

    for i, chunk in enumerate(raws):
        raw_move(0, chunk, 0, to_x).wait_recv()
        if i % 2 == 0:
            go(raw_move(5, chunk, 0, to_y))
        raw_move(1, chunk, 0, to_y).wait_recv()
        if i % 2 == 1:
            go(raw_move(5, chunk, 1, to_x))
    correct(0, to_x)
    correct(1, to_y)

    def relay(i, chunk, forward):
        move(0, chunk, to_x, to_x).wait_recv()
        if i % 2 == 0:
            go(move(5, chunk, to_x, to_y))
        if forward:
            go(move(3, chunk, to_x, sib))
        move(1, chunk, to_y, to_y).wait_recv()
        if i % 2 == 1:
            go(move(5, chunk, to_y, to_x))
        if forward:
            go(move(4, chunk, to_y, sib))

    for i, chunk in enumerate(bulk):
        relay(i, chunk, True)
        if i == 0:
            go(move(3, block, to_x, sib))
            go(move(4, block, to_y, sib))

    for chunk in raws:
        raw_move(5, chunk, 0, to_x).wait_recv()
    small(far_l.at[0], far_l.at[2], 6, to_y).wait_recv()
    small(far_g.at[0], far_g.at[2], 9, to_y).wait_recv()
    correct(2, diag)
    for i, chunk in enumerate(bulk):
        move(5, chunk, diag, to_x).wait_recv()
        go(move(6, chunk, diag, sib))
        if i == 0:
            go(move(6, block, diag, sib))
        if i == 0:
            @pl.when(core == late)
            def _():
                for chunk in alone:
                    move(0, chunk, me, to_x).start()
                    move(1, chunk, me, to_y).start()
    arrived = 3 * early + sum(3 * z for _, _, z in bulk) + rows + rows
    all_of(arrived, 2).wait_recv()

    @pl.when(core == late)
    def _():
        for i, chunk in enumerate(alone):
            relay(i, chunk, False)
        for chunk in alone:
            move(5, chunk, diag, to_x).wait_recv()
        all_of(3 * solo, 1).wait_send()
        sum_pair.wait_send()

    @pl.when(core != late)
    def _():
        small(heard, heard, 0, sib).wait_send()

    all_of(3 * sum(z for _, _, z in every), 0).wait_send()
    all_of(arrived, 2).wait_send()
    small(far_l, far_l, 4, to_x).wait_send()
    small(far_g, far_g, 7, to_x).wait_send()


def tail_kernel(rows, unit, up, after, tail, ready, sent, crossed, recv):
    solo = tail.shape[1]
    me, core, sib, to_x, to_y, diag, flip = place()
    chunks = pairs(0, unit, ALONE)
    whole = (0, solo)
    rest = (to_x, to_y, diag)
    barrier = pltpu.get_barrier_semaphore()

    lanes = {0: 0, 1: 1, 5: 2}

    def remote(src, dst, slot, i, target):
        inner = slot in lanes
        return pltpu.make_async_remote_copy(
            src_ref=src, dst_ref=dst, send_sem=sent.at[0 if inner else 1],
            recv_sem=recv.at[lanes[slot], i] if inner else crossed, device_id={AXIS: target})

    def all_of(out):
        part = tail.at[0:3]
        return pltpu.make_async_remote_copy(
            src_ref=part, dst_ref=part, send_sem=sent.at[out], recv_sem=crossed,
            device_id={AXIS: sib})

    def held(owner, s, z):
        return up.at[pl.ds(pl.multiple_of(owner * rows + rows - solo + s, 8), z), :]

    def move(slot, i, chunk, owner, target, first=False):
        s, z = chunk
        dst = tail.at[owner, s:s + z, :]
        return remote(held(owner, s, z) if first else dst, dst, slot, i, target)

    def go(c):
        c.start()

    @pl.when(core != late)
    def _():
        for d in (to_x, to_y, sib):
            pl.semaphore_signal(barrier, inc=1, device_id={AXIS: d})
        pl.semaphore_wait(barrier, 2)
        for i, c in enumerate(chunks):
            go(move(0, i, c, me, to_x, True))
            go(move(1, i, c, me, to_y, True))
        for i, c in enumerate(chunks):
            move(0, i, c, to_x, to_x).wait_recv()
            if i % 2 == 0:
                go(move(5, i, c, to_x, to_y))
            move(1, i, c, to_y, to_y).wait_recv()
            if i % 2 == 1:
                go(move(5, i, c, to_y, to_x))
        pl.semaphore_wait(ready, 1)
        go(move(3, 0, whole, to_x, sib))
        go(move(4, 0, whole, to_y, sib))
        for i, c in enumerate(chunks):
            move(5, i, c, diag, to_x).wait_recv()
            go(move(6, i, c, diag, sib))
        all_of(0).wait_send()

    @pl.when(core == late)
    def _():
        pl.semaphore_wait(barrier, 1)
        pl.semaphore_signal(ready, inc=1, device_id={AXIS: sib})
        for i, owner in enumerate(rest):
            go(move(7, i, whole, owner, sib, True))

    all_of(1).wait_recv()
    all_of(1).wait_send()


def write_kernel(rows, solo, a_v, b_v, fac, a_hbm, b_hbm, fa_hbm, fb_hbm, done, sem):
    done[...] = jnp.zeros_like(done)
    n = a_v.shape[0] // rows
    first = lax.axis_index(AXIS) // 2 * 2
    waits = [
        pltpu.make_async_copy(fac.at[i, 0], dst, sem.at[i])
        for i, dst in enumerate((fa_hbm, fb_hbm))
    ]
    for c in waits:
        c.start()
    for k in range(n):
        for i, (src, dst) in enumerate(((a_v, a_hbm), (b_v, b_hbm))):
            owner = lax.rem(first + k, n)
            z = rows - solo if i and k > 1 else rows
            r = pl.ds(pl.multiple_of(owner * rows, 8), z)
            pltpu.make_async_copy(src.at[r, :], dst.at[r, :], sem.at[2 + i]).start()
    me = lax.axis_index(AXIS)
    alone = lax.rem(me, 2) == late

    @pl.when(alone)
    def _():
        for k in range(2, n, 2):
            r = pl.ds(pl.multiple_of((lax.rem(me + k, n) + 1) * rows - solo, 8), solo)
            pltpu.make_async_copy(b_v.at[r, :], b_hbm.at[r, :], sem.at[4]).start()

    waits.append(pltpu.make_async_copy(a_v, a_hbm, sem.at[2]))
    r = pl.ds(0, n * rows - (n - 2) * solo)
    waits.append(pltpu.make_async_copy(b_v.at[r, :], b_hbm.at[r, :], sem.at[3]))
    for c in waits:
        c.wait()

    @pl.when(alone)
    def _():
        part = b_hbm.at[0:(n // 2 - 1) * solo, :]
        pltpu.make_async_copy(part, part, sem.at[4]).wait()


def finish_kernel(rows, tail, before, b_hbm, sem):
    n, solo, _ = tail.shape
    me = lax.axis_index(AXIS)
    first = me // 2 * 2
    part = b_hbm.at[0:(n // 2 - 1) * solo, :]

    def write(side):
        for k in range(2, n, 2):
            owner = lax.rem(first + k + side, n)
            r = pl.ds(pl.multiple_of((owner + 1) * rows - solo, 8), solo)
            pltpu.make_async_copy(tail.at[owner], b_hbm.at[r, :], sem.at[side]).start()

    def wait(side):
        pltpu.make_async_copy(part, part, sem.at[side]).wait()

    write(1 - late)
    own = lax.rem(me, 2) == late

    @pl.when(jnp.logical_not(own))
    def _():
        write(late)
        wait(late)

    wait(1 - late)


def paired(n, weight_gate, low_gate, high_gate, weight_up, low_up, high_up, norm_gain):
    rows, cols = weight_gate.shape
    unit = rows // 40
    solo = 2 * sum(ALONE) * unit
    early = 2 * sum(RAW) * unit
    full = (n * rows, cols)
    vmem = pl.BlockSpec(memory_space=pltpu.VMEM)
    hbm = pl.BlockSpec(memory_space=pl.ANY)
    space = pl.BlockSpec(memory_space=pltpu.HBM)
    rank = high_gate.shape[0]
    grant = 65472 * 2**10 - (4 * full[0] * cols + 8 * cols) // 2**10 * 2**10 - 24 * 2**10
    moves = 2 * (len(RAW) + len(GATE) + len(UP) + len(ALONE))
    gate, up, fac = pl.pallas_call(
        functools.partial(gather_kernel, unit, solo),
        out_shape=(
            pltpu.VMEM(full, jnp.bfloat16),
            pltpu.VMEM(full, jnp.bfloat16),
            pltpu.VMEM((2, 1, cols), jnp.float32),
        ),
        in_specs=[space] * 7,
        out_specs=(vmem, vmem, vmem),
        scratch_shapes=[
            pltpu.VMEM((2, rows, cols), jnp.bfloat16),
            pltpu.VMEM((2, rank, rows), jnp.bfloat16),
            pltpu.VMEM((2, rank, cols), jnp.bfloat16),
            pltpu.VMEM((1, rows), jnp.float32),
            pltpu.VMEM((2, rows, rank), jnp.bfloat16),
            pltpu.VMEM((2, rows, cols), jnp.float32),
            pltpu.VMEM((rows, 128), jnp.float32),
            pltpu.VMEM((2, 1, cols), jnp.float32),
            pltpu.VMEM((3, 2, 1, cols), jnp.float32),
            pltpu.VMEM((3, 2, 1, cols), jnp.float32),
            pltpu.VMEM((2, 1, cols), jnp.float32),
            pltpu.VMEM((3, early, cols), jnp.bfloat16),
            pltpu.VMEM((3, rank, early), jnp.bfloat16),
            pltpu.VMEM((3, 1, early), jnp.float32),
            pltpu.VMEM((3, early, rank), jnp.bfloat16),
            pltpu.VMEM((3, early, 128), jnp.float32),
            pltpu.SemaphoreType.DMA((7 + 2 * len(RAW),)),
            pltpu.SemaphoreType.DMA((3,)),
            pltpu.SemaphoreType.DMA((10,)),
            pltpu.SemaphoreType.DMA((3,)),
            pltpu.SemaphoreType.DMA,
            pltpu.SemaphoreType.DMA((3, moves)),
        ],
        compiler_params=pltpu.CompilerParams(
            collective_id=0, has_side_effects=True, vmem_limit_bytes=grant
        ),
        name="merge_gather",
    )(weight_gate, weight_up, low_gate.T, low_up.T, high_gate, high_up, norm_gain)
    whole = jax.ShapeDtypeStruct(full, jnp.bfloat16)
    ready_gate, ready_up, factor_gate, factor_up, done = pl.pallas_call(
        functools.partial(write_kernel, rows, solo),
        out_shape=(whole, whole) + (jax.ShapeDtypeStruct((cols,), jnp.float32),) * 2
        + (pltpu.VMEM((8, 128), jnp.float32),),
        in_specs=[vmem, vmem, vmem],
        out_specs=(hbm,) * 4 + (vmem,),
        scratch_shapes=[pltpu.SemaphoreType.DMA((5,))],
        compiler_params=pltpu.CompilerParams(vmem_limit_bytes=2**20),
        name="write_out",
    )(gate, up, fac)
    tail = pl.pallas_call(
        functools.partial(tail_kernel, rows, unit),
        out_shape=pltpu.VMEM((n, solo, cols), jnp.bfloat16),
        in_specs=[vmem, vmem],
        out_specs=vmem,
        scratch_shapes=[
            pltpu.SemaphoreType.REGULAR,
            pltpu.SemaphoreType.DMA((2,)),
            pltpu.SemaphoreType.DMA,
            pltpu.SemaphoreType.DMA((3, 2 * len(ALONE))),
        ],
        compiler_params=pltpu.CompilerParams(
            collective_id=1, has_side_effects=True, vmem_limit_bytes=2**20
        ),
        name="tail_gather",
    )(up, done)
    ready_up = pl.pallas_call(
        functools.partial(finish_kernel, rows),
        out_shape=whole,
        in_specs=[vmem, hbm],
        out_specs=hbm,
        input_output_aliases={1: 0},
        scratch_shapes=[pltpu.SemaphoreType.DMA((2,))],
        compiler_params=pltpu.CompilerParams(vmem_limit_bytes=2**20),
        name="finish",
    )(tail, ready_up)
    return ready_gate, ready_up, factor_gate, factor_up


def solution(mesh):
    in_specs = (
        P("shard", "tp"),
        P("shard", None),
        P(None, "tp"),
        P("shard", "tp"),
        P("shard", None),
        P(None, "tp"),
        P("shard"),
    )
    out_specs = (P(None, "tp"), P(None, "tp"), P("tp"), P("tp"))
    n = mesh.shape[AXIS]
    side = math.isqrt(n // 2)
    body = functools.partial(paired, n) if side == 2 and 2 * side * side == n else local
    return jax.shard_map(body, mesh=mesh, in_specs=in_specs, out_specs=out_specs, check_vma=False)
```

```python
import functools
import math

import jax
import jax.numpy as jnp
from jax import lax
from jax.experimental import pallas as pl
from jax.experimental.pallas import tpu as pltpu
from jax.sharding import PartitionSpec as P

mix_rate = 2.0
AXIS = "shard"


def local(weight_gate, low_gate, high_gate, weight_up, low_up, high_up, norm_gain):
    latest_gate = weight_gate.astype(jnp.float32) + mix_rate * jnp.dot(
        low_gate, high_gate, preferred_element_type=jnp.float32
    )
    latest_up = weight_up.astype(jnp.float32) + mix_rate * jnp.dot(
        low_up, high_up, preferred_element_type=jnp.float32
    )
    latest_gained_gate = latest_gate * norm_gain[:, None]
    latest_gained_up = latest_up * norm_gain[:, None]
    total_gate, total_up = lax.psum(
        (
            jnp.sum(latest_gained_gate * latest_gained_gate, axis=0),
            jnp.sum(latest_gained_up * latest_gained_up, axis=0),
        ),
        AXIS,
    )
    factor_gate = jnp.sqrt(total_gate)
    factor_up = jnp.sqrt(total_up)
    narrow_gate = (latest_gained_gate / factor_gate).astype(jnp.bfloat16)
    narrow_up = (latest_gained_up / factor_up).astype(jnp.bfloat16)
    ready_gate = lax.all_gather(narrow_gate, AXIS, axis=0, tiled=True)
    ready_up = lax.all_gather(narrow_up, AXIS, axis=0, tiled=True)
    return (ready_gate, ready_up, factor_gate, factor_up)


late = 0
RAW = (2, 6)
GATE = (12,)
UP = (10,)
ALONE = (4, 4, 2)


def place():
    me = lax.axis_index(AXIS)
    core = lax.rem(me, 2)
    x = lax.rem(me // 2, 2)
    y = me // 4
    to_x = me + 2 - 4 * x
    to_y = me + 4 - 8 * y
    return me, core, me + 1 - 2 * core, to_x, to_y, to_x + 4 - 8 * y, 1 - 2 * core


def pairs(start, unit, sizes):
    out = []
    for z in sizes:
        for _ in range(2):
            out.append((start, z * unit))
            start += z * unit
    return out


def gather_kernel(
    unit, solo, wg_hbm, wu_hbm, lg_hbm, lu_hbm, hg_hbm, hu_hbm, gain_hbm,
    out_g, out_u, fac,
    w_v, l_v, h_v, gain_v, low_v, g_v, col_v, part, mine, heard, rf_v,
    raw_v, far_l, far_g, far_low, far_col,
    in_sem, small_send, small_recv, sent, crossed, recv,
):
    rows, cols = wg_hbm.shape
    me, core, sib, to_x, to_y, diag, flip = place()
    early = 2 * sum(RAW) * unit
    shared_up = rows - solo
    raws = [(0, s, z) for s, z in pairs(0, unit, RAW)]
    bulk = [(0, s, z) for s, z in pairs(early, unit, GATE)]
    bulk += [(1, s, z) for s, z in pairs(0, unit, UP)]
    alone = [(1, s, z) for s, z in pairs(shared_up, unit, ALONE)]
    own_tail = (1, shared_up, solo)
    block = (0, 0, early)
    every = raws + bulk
    order = {c: i for i, c in enumerate(every + alone)}
    lanes = {0: 0, 1: 1, 5: 2}
    outs = (out_g, out_u)

    barrier = pltpu.get_barrier_semaphore()
    for d in (to_x, to_y, sib):
        pl.semaphore_signal(barrier, inc=1, device_id={AXIS: d})

    gain_load = pltpu.make_async_copy(gain_hbm, gain_v.at[0], in_sem.at[6])
    low_loads, high_loads = (
        [
            pltpu.make_async_copy(src, dst.at[a], in_sem.at[3 * a + i])
            for a, src in enumerate(pair)
        ]
        for i, (pair, dst) in enumerate((((lg_hbm, lu_hbm), l_v), ((hg_hbm, hu_hbm), h_v)))
    )
    loads = [
        pltpu.make_async_copy(wg_hbm.at[early:, :], w_v.at[0, early:, :], in_sem.at[2]),
        pltpu.make_async_copy(wu_hbm, w_v.at[1], in_sem.at[5]),
    ]
    raw_loads = [
        pltpu.make_async_copy(wg_hbm.at[s:s + z, :], w_v.at[0, s:s + z, :], in_sem.at[7 + i])
        for i, (_, s, z) in enumerate(raws)
    ]
    for c in raw_loads[:2] + [low_loads[0], gain_load, high_loads[0]] + raw_loads[2:]:
        c.start()
    for c in (loads[0], low_loads[1], high_loads[1], loads[1]):
        c.start()

    def go(c):
        c.start()

    def remote(src, dst, slot, chunk, target):
        if slot in lanes:
            got = recv.at[lanes[slot], order[chunk]]
            out = sent.at[1 if chunk in alone else 0]
        else:
            got, out = crossed, sent.at[2]
        return pltpu.make_async_remote_copy(
            src_ref=src, dst_ref=dst, send_sem=out, recv_sem=got, device_id={AXIS: target})

    def all_of(count, out):
        part = out_g.at[0:count, :]
        return pltpu.make_async_remote_copy(
            src_ref=part, dst_ref=part, send_sem=sent.at[out], recv_sem=crossed,
            device_id={AXIS: sib})

    def small(src, dst, i, target):
        return pltpu.make_async_remote_copy(
            src_ref=src, dst_ref=dst, send_sem=small_send.at[(i >= 4) + (i >= 7)],
            recv_sem=small_recv.at[i], device_id={AXIS: target})

    def piece(chunk, owner):
        a, s, z = chunk
        return outs[a].at[pl.ds(pl.multiple_of(owner * rows + s, 8), z), :]

    def move(slot, chunk, owner, target):
        p = piece(chunk, owner)
        return remote(p, p, slot, chunk, target)

    def raw_move(slot, chunk, at, target):
        _, s, z = chunk
        src = w_v.at[0, s:s + z, :] if slot < 2 else raw_v.at[at, s:s + z, :]
        return remote(src, raw_v.at[slot if slot < 2 else 2, s:s + z, :], slot, chunk, target)

    pl.semaphore_wait(barrier, 3)
    for c, chunk in list(zip(raw_loads, raws))[:2]:
        c.wait()
        go(raw_move(0, chunk, 0, to_x))
        go(raw_move(1, chunk, 0, to_y))
    low_own, gain_own = l_v.at[0, :, :early], gain_v.at[:, :early]
    low_loads[0].wait()
    gain_load.wait()
    for i, d in enumerate((to_x, to_y)):
        go(small(low_own, far_l.at[i], 4 + i, d))
        go(small(gain_own, far_g.at[i], 7 + i, d))

    col_v[...] = jnp.broadcast_to(gain_v[...], (128, rows)).T
    step = rows // 5
    for a in range(2):
        if a:
            low_loads[a].wait()
        else:
            for c in raw_loads[2:]:
                c.wait()
        low_v[a] = (mix_rate * l_v[a].astype(jnp.float32)).T.astype(jnp.bfloat16)
        high_loads[a].wait()
        loads[a].wait()
        acc = jnp.zeros((8, cols), jnp.float32)
        for s in range(0, rows, step):
            r = pl.ds(s, step)
            prod = jnp.dot(low_v[a, r, :], h_v[a], preferred_element_type=jnp.float32)
            new = (w_v[a, r, :].astype(jnp.float32) + prod) * col_v[r, 0:1]
            g_v[a, r, :] = new
            acc = acc + jnp.sum((new * new).reshape(step // 8, 8, cols), axis=0)
        part[a] = jnp.sum(acc, axis=0, keepdims=True)

    sum_pair = small(part, heard.at[0], 0, sib)
    sum_x = small(mine.at[0], heard.at[1], 1, to_x)
    sum_y = small(mine.at[1], heard.at[2], 2, to_y)
    sum_all = small(mine.at[2], mine.at[2], 3, sib)

    @pl.when(core == late)
    def _():
        sum_pair.start()
        for chunk in raws[2:]:
            raw_move(0, chunk, 0, to_x).start()
            raw_move(1, chunk, 0, to_y).start()
        sum_all.wait_recv()

    @pl.when(core != late)
    def _():
        sum_pair.wait_recv()
        mine[0] = part[...] + heard[0]
        raw_move(1, raws[2], 0, to_y).start()
        sum_x.start()
        raw_move(0, raws[2], 0, to_x).start()
        sum_x.wait_recv()
        mine[1] = mine[0] + heard[1]
        raw_move(0, raws[3], 0, to_x).start()
        sum_y.start()
        raw_move(1, raws[3], 0, to_y).start()
        sum_y.wait_recv()
        mine[2] = mine[1] + heard[2]
        sum_all.start()

    for a in range(2):
        factor = jnp.sqrt(mine[2, a])
        fac[a] = factor
        rf_v[a] = 1.0 / factor

    def scale(chunk):
        a, s, z = chunk
        r = pl.ds(pl.multiple_of(me * rows + s, 8), z)
        outs[a][r, :] = (g_v[a, s:s + z, :] * rf_v[a]).astype(jnp.bfloat16)

    def send_own(chunk):
        go(move(0, chunk, me, to_x))
        go(move(1, chunk, me, to_y))
        go(move(2, chunk, me, sib))

    for i, chunk in enumerate(bulk):
        scale(chunk)
        if i:
            send_own(bulk[i - 1])
    scale(block)
    send_own(bulk[-1])
    for chunk in alone:
        scale(chunk)
    go(move(2, block, me, sib))
    go(move(2, own_tail, me, sib))

    low_x, low_y = (small(low_own, far_l.at[i], 4 + i, to_x) for i in range(2))
    gain_x, gain_y = (small(gain_own, far_g.at[i], 7 + i, to_x) for i in range(2))
    for c in (low_x, low_y, gain_x, gain_y):
        c.wait_recv()
    over = to_y + core * (to_x - to_y)
    go(small(far_l.at[core], far_l.at[2], 6, over))
    go(small(far_g.at[core], far_g.at[2], 9, over))

    def correct(i, owner):
        far_low[i] = (mix_rate * far_l[i].astype(jnp.float32)).T.astype(jnp.bfloat16)
        far_col[i] = jnp.broadcast_to(far_g[i], (128, early)).T
        for s in range(0, early, early // 2):
            r = pl.ds(s, early // 2)
            prod = jnp.dot(far_low[i, r, :], h_v[0], preferred_element_type=jnp.float32)
            new = (raw_v[i, r, :].astype(jnp.float32) + prod) * far_col[i, r, 0:1]
            o = pl.ds(pl.multiple_of(owner * rows + s, 8), early // 2)
            out_g[o, :] = (new * rf_v[0]).astype(jnp.bfloat16)

    for i, chunk in enumerate(raws):
        raw_move(0, chunk, 0, to_x).wait_recv()
        if i % 2 == 0:
            go(raw_move(5, chunk, 0, to_y))
        raw_move(1, chunk, 0, to_y).wait_recv()
        if i % 2 == 1:
            go(raw_move(5, chunk, 1, to_x))
    correct(0, to_x)
    correct(1, to_y)

    def relay(i, chunk, forward):
        move(0, chunk, to_x, to_x).wait_recv()
        if i % 2 == 0:
            go(move(5, chunk, to_x, to_y))
        if forward:
            go(move(3, chunk, to_x, sib))
        move(1, chunk, to_y, to_y).wait_recv()
        if i % 2 == 1:
            go(move(5, chunk, to_y, to_x))
        if forward:
            go(move(4, chunk, to_y, sib))

    for i, chunk in enumerate(bulk):
        relay(i, chunk, True)
        if i == 0:
            go(move(3, block, to_x, sib))
            go(move(4, block, to_y, sib))

    for chunk in raws:
        raw_move(5, chunk, 0, to_x).wait_recv()
    small(far_l.at[0], far_l.at[2], 6, to_y).wait_recv()
    small(far_g.at[0], far_g.at[2], 9, to_y).wait_recv()
    correct(2, diag)
    for i, chunk in enumerate(bulk):
        move(5, chunk, diag, to_x).wait_recv()
        go(move(6, chunk, diag, sib))
        if i == 0:
            go(move(6, block, diag, sib))
        if i == 0:
            @pl.when(core == late)
            def _():
                for chunk in alone:
                    move(0, chunk, me, to_x).start()
                    move(1, chunk, me, to_y).start()
    arrived = 3 * early + sum(3 * z for _, _, z in bulk) + rows + rows
    all_of(arrived, 2).wait_recv()

    @pl.when(core == late)
    def _():
        for i, chunk in enumerate(alone):
            relay(i, chunk, False)
        for chunk in alone:
            move(5, chunk, diag, to_x).wait_recv()
        all_of(3 * solo, 1).wait_send()
        sum_pair.wait_send()

    @pl.when(core != late)
    def _():
        small(heard, heard, 0, sib).wait_send()

    all_of(3 * sum(z for _, _, z in every), 0).wait_send()
    all_of(arrived, 2).wait_send()
    small(far_l, far_l, 4, to_x).wait_send()
    small(far_g, far_g, 7, to_x).wait_send()


def tail_kernel(rows, unit, up, after, tail, ready, sent, crossed, recv):
    solo = tail.shape[1]
    me, core, sib, to_x, to_y, diag, flip = place()
    chunks = pairs(0, unit, ALONE)
    whole = (0, solo)
    rest = (to_x, to_y, diag)
    barrier = pltpu.get_barrier_semaphore()

    lanes = {0: 0, 1: 1, 5: 2}

    def remote(src, dst, slot, i, target):
        inner = slot in lanes
        return pltpu.make_async_remote_copy(
            src_ref=src, dst_ref=dst, send_sem=sent.at[0 if inner else 1],
            recv_sem=recv.at[lanes[slot], i] if inner else crossed, device_id={AXIS: target})

    def all_of(out):
        part = tail.at[0:3]
        return pltpu.make_async_remote_copy(
            src_ref=part, dst_ref=part, send_sem=sent.at[out], recv_sem=crossed,
            device_id={AXIS: sib})

    def held(owner, s, z):
        return up.at[pl.ds(pl.multiple_of(owner * rows + rows - solo + s, 8), z), :]

    def move(slot, i, chunk, owner, target, first=False):
        s, z = chunk
        dst = tail.at[owner, s:s + z, :]
        return remote(held(owner, s, z) if first else dst, dst, slot, i, target)

    def go(c):
        c.start()

    @pl.when(core != late)
    def _():
        for d in (to_x, to_y, sib):
            pl.semaphore_signal(barrier, inc=1, device_id={AXIS: d})
        pl.semaphore_wait(barrier, 2)
        for i, c in enumerate(chunks):
            go(move(0, i, c, me, to_x, True))
            go(move(1, i, c, me, to_y, True))
        for i, c in enumerate(chunks):
            move(0, i, c, to_x, to_x).wait_recv()
            if i % 2 == 0:
                go(move(5, i, c, to_x, to_y))
            move(1, i, c, to_y, to_y).wait_recv()
            if i % 2 == 1:
                go(move(5, i, c, to_y, to_x))
        pl.semaphore_wait(ready, 1)
        go(move(3, 0, whole, to_x, sib))
        go(move(4, 0, whole, to_y, sib))
        for i, c in enumerate(chunks):
            move(5, i, c, diag, to_x).wait_recv()
            go(move(6, i, c, diag, sib))
        all_of(0).wait_send()

    @pl.when(core == late)
    def _():
        pl.semaphore_wait(barrier, 1)
        pl.semaphore_signal(ready, inc=1, device_id={AXIS: sib})
        for i, owner in enumerate(rest):
            go(move(7, i, whole, owner, sib, True))

    all_of(1).wait_recv()
    all_of(1).wait_send()


def write_kernel(rows, solo, a_v, b_v, fac, a_hbm, b_hbm, fa_hbm, fb_hbm, done, sem):
    done[...] = jnp.zeros_like(done)
    n = a_v.shape[0] // rows
    first = lax.axis_index(AXIS) // 2 * 2
    waits = [
        pltpu.make_async_copy(fac.at[i, 0], dst, sem.at[i])
        for i, dst in enumerate((fa_hbm, fb_hbm))
    ]
    for c in waits:
        c.start()
    for k in range(n):
        for i, (src, dst) in enumerate(((a_v, a_hbm), (b_v, b_hbm))):
            owner = lax.rem(first + k, n)
            z = rows - solo if i and k > 1 else rows
            r = pl.ds(pl.multiple_of(owner * rows, 8), z)
            pltpu.make_async_copy(src.at[r, :], dst.at[r, :], sem.at[2 + i]).start()
    me = lax.axis_index(AXIS)
    alone = lax.rem(me, 2) == late

    @pl.when(alone)
    def _():
        for k in range(2, n, 2):
            r = pl.ds(pl.multiple_of((lax.rem(me + k, n) + 1) * rows - solo, 8), solo)
            pltpu.make_async_copy(b_v.at[r, :], b_hbm.at[r, :], sem.at[4]).start()

    waits.append(pltpu.make_async_copy(a_v, a_hbm, sem.at[2]))
    r = pl.ds(0, n * rows - (n - 2) * solo)
    waits.append(pltpu.make_async_copy(b_v.at[r, :], b_hbm.at[r, :], sem.at[3]))
    for c in waits:
        c.wait()

    @pl.when(alone)
    def _():
        part = b_hbm.at[0:(n // 2 - 1) * solo, :]
        pltpu.make_async_copy(part, part, sem.at[4]).wait()


def finish_kernel(rows, tail, before, b_hbm, sem):
    n, solo, _ = tail.shape
    me = lax.axis_index(AXIS)
    first = me // 2 * 2
    part = b_hbm.at[0:(n // 2 - 1) * solo, :]

    def write(side):
        for k in range(2, n, 2):
            owner = lax.rem(first + k + side, n)
            r = pl.ds(pl.multiple_of((owner + 1) * rows - solo, 8), solo)
            pltpu.make_async_copy(tail.at[owner], b_hbm.at[r, :], sem.at[side]).start()

    def wait(side):
        pltpu.make_async_copy(part, part, sem.at[side]).wait()

    write(1 - late)
    own = lax.rem(me, 2) == late

    @pl.when(jnp.logical_not(own))
    def _():
        write(late)
        wait(late)

    wait(1 - late)


def paired(n, weight_gate, low_gate, high_gate, weight_up, low_up, high_up, norm_gain):
    rows, cols = weight_gate.shape
    unit = rows // 40
    solo = 2 * sum(ALONE) * unit
    early = 2 * sum(RAW) * unit
    full = (n * rows, cols)
    vmem = pl.BlockSpec(memory_space=pltpu.VMEM)
    hbm = pl.BlockSpec(memory_space=pl.ANY)
    space = pl.BlockSpec(memory_space=pltpu.HBM)
    rank = high_gate.shape[0]
    grant = 65472 * 2**10 - (4 * full[0] * cols + 8 * cols) // 2**10 * 2**10 - 24 * 2**10
    moves = 2 * (len(RAW) + len(GATE) + len(UP) + len(ALONE))
    gate, up, fac = pl.pallas_call(
        functools.partial(gather_kernel, unit, solo),
        out_shape=(
            pltpu.VMEM(full, jnp.bfloat16),
            pltpu.VMEM(full, jnp.bfloat16),
            pltpu.VMEM((2, 1, cols), jnp.float32),
        ),
        in_specs=[space] * 7,
        out_specs=(vmem, vmem, vmem),
        scratch_shapes=[
            pltpu.VMEM((2, rows, cols), jnp.bfloat16),
            pltpu.VMEM((2, rank, rows), jnp.bfloat16),
            pltpu.VMEM((2, rank, cols), jnp.bfloat16),
            pltpu.VMEM((1, rows), jnp.float32),
            pltpu.VMEM((2, rows, rank), jnp.bfloat16),
            pltpu.VMEM((2, rows, cols), jnp.float32),
            pltpu.VMEM((rows, 128), jnp.float32),
            pltpu.VMEM((2, 1, cols), jnp.float32),
            pltpu.VMEM((3, 2, 1, cols), jnp.float32),
            pltpu.VMEM((3, 2, 1, cols), jnp.float32),
            pltpu.VMEM((2, 1, cols), jnp.float32),
            pltpu.VMEM((3, early, cols), jnp.bfloat16),
            pltpu.VMEM((3, rank, early), jnp.bfloat16),
            pltpu.VMEM((3, 1, early), jnp.float32),
            pltpu.VMEM((3, early, rank), jnp.bfloat16),
            pltpu.VMEM((3, early, 128), jnp.float32),
            pltpu.SemaphoreType.DMA((7 + 2 * len(RAW),)),
            pltpu.SemaphoreType.DMA((3,)),
            pltpu.SemaphoreType.DMA((10,)),
            pltpu.SemaphoreType.DMA((3,)),
            pltpu.SemaphoreType.DMA,
            pltpu.SemaphoreType.DMA((3, moves)),
        ],
        compiler_params=pltpu.CompilerParams(
            collective_id=0, has_side_effects=True, vmem_limit_bytes=grant
        ),
        name="merge_gather",
    )(weight_gate, weight_up, low_gate.T, low_up.T, high_gate, high_up, norm_gain)
    whole = jax.ShapeDtypeStruct(full, jnp.bfloat16)
    ready_gate, ready_up, factor_gate, factor_up, done = pl.pallas_call(
        functools.partial(write_kernel, rows, solo),
        out_shape=(whole, whole) + (jax.ShapeDtypeStruct((cols,), jnp.float32),) * 2
        + (pltpu.VMEM((8, 128), jnp.float32),),
        in_specs=[vmem, vmem, vmem],
        out_specs=(hbm,) * 4 + (vmem,),
        scratch_shapes=[pltpu.SemaphoreType.DMA((5,))],
        compiler_params=pltpu.CompilerParams(vmem_limit_bytes=2**20),
        name="write_out",
    )(gate, up, fac)
    tail = pl.pallas_call(
        functools.partial(tail_kernel, rows, unit),
        out_shape=pltpu.VMEM((n, solo, cols), jnp.bfloat16),
        in_specs=[vmem, vmem],
        out_specs=vmem,
        scratch_shapes=[
            pltpu.SemaphoreType.REGULAR,
            pltpu.SemaphoreType.DMA((2,)),
            pltpu.SemaphoreType.DMA,
            pltpu.SemaphoreType.DMA((3, 2 * len(ALONE))),
        ],
        compiler_params=pltpu.CompilerParams(
            collective_id=1, has_side_effects=True, vmem_limit_bytes=2**20
        ),
        name="tail_gather",
    )(up, done)
    ready_up = pl.pallas_call(
        functools.partial(finish_kernel, rows),
        out_shape=whole,
        in_specs=[vmem, hbm],
        out_specs=hbm,
        input_output_aliases={1: 0},
        scratch_shapes=[pltpu.SemaphoreType.DMA((2,))],
        compiler_params=pltpu.CompilerParams(vmem_limit_bytes=2**20),
        name="finish",
    )(tail, ready_up)
    return ready_gate, ready_up, factor_gate, factor_up


def solution(mesh):
    in_specs = (
        P("shard", "tp"),
        P("shard", None),
        P(None, "tp"),
        P("shard", "tp"),
        P("shard", None),
        P(None, "tp"),
        P("shard"),
    )
    out_specs = (P(None, "tp"), P(None, "tp"), P("tp"), P("tp"))
    n = mesh.shape[AXIS]
    side = math.isqrt(n // 2)
    body = functools.partial(paired, n) if side == 2 and 2 * side * side == n else local
    return jax.shard_map(body, mesh=mesh, in_specs=in_specs, out_specs=out_specs, check_vma=False)
```
